32 devices in a mesh: flow: 8 (over z, x), leaf: 4 (over y, core).
Axes of the slice: x: 2, y: 2, z: 4, core: 2. Of those that a mesh axis runs over, the one named last changes fastest.
Arguments:
- vel_coef: float32 [81, 16384], P(None, 'flow'), may hold values from -6 to 6
- gp_block: int32 [65536, 1], P(('flow', 'leaf')), may hold values from 0 to 7; in each aligned block of 2048 rows (0 to 2047, 2048 to 4095, ...) at most 512 rows name the same one
- gp_elem: int32 [65536], P(('flow', 'leaf')), may hold values from 0 to 2047
- gp_param: float32 [3, 65536], P(None, ('flow', 'leaf')), may hold values from 0 to 1
- gp_vel: float32 [3, 65536], P(None, ('flow', 'leaf')), may hold values from -6 to 6
- gp_weight: float32 [65536], P(('flow', 'leaf')), may hold values from 0.1 to 1
- gp_pos: float32 [3, 65536], P(None, ('flow', 'leaf')), may hold values from -4 to 4
- contact_patch: int32 [65536], P(('flow', 'leaf')), may hold values from 0 to 1023
- contact_param: float32 [2, 65536], P(None, ('flow', 'leaf')), may hold values from 0 to 1
- patch_ctrl: float32 [27, 8192], P(None, ('flow', 'leaf')), may hold values from -4 to 4
Outputs:
- flow_force: float32 [81, 16384], P(None, ('flow', 'leaf'))
- shell_force: float32 [3, 65536], P(None, ('flow', 'leaf'))
- patch_force: float32 [27, 8192], P(None, ('flow', 'leaf'))
The draws below stay inside these ranges and needn't reach their ends.
Inputs may be any that keep to these rules, and one draw needn't show every extreme that they name: `gp_block`: the Gauss points of one device lie in at most 512 of each flow block's elements; some block is reached with exactly 512. `contact_patch`: A contact partner is one of the 1024 patches held by the Gauss point's own group, the devices of one index of flow.
All inputs are finite; a program needn't handle non-finite values.
Results may differ from the reference program's by a relative error of at most 0.0001.
Values sent between devices are 32-bit elements; how exact they have to be, the bound alone decides.
No kernel may reach another device: no remote copies, remote signals or barrier semaphores. Data moves between devices by JAX's collectives and lax.ppermute only.
A program may use at most 64 MiB of HBM per device.

```python
import math
import jax
import jax.numpy as jnp
import numpy as np

E_DEV = 2048
GP_DEV = 2048
CAP = 512
NELEM = 16384
GP = 65536
NP_GROUP = 1024
NPATCH = 8192
N_FLOW = 8
N_LEAF = 4


def with_ends(array, stream_key, least, high):
    extent = array.shape
    spot = [jax.random.randint(jax.random.fold_in(stream_key, axis), (), 0, extent[axis]) for axis in range(len(extent))]
    array = array.at[tuple(spot)].set(least)
    longest = extent.index(max(extent))
    spot[longest] = (spot[longest] + 1) % extent[longest]
    return array.at[tuple(spot)].set(high)


def level_of(key, extent, pieces, low, largest):
    def one(dim, shards_of):
        steps = jax.random.uniform(jax.random.fold_in(jax.random.fold_in(key, 6), dim), (shards_of,), jnp.float32, low / len(pieces), largest / len(pieces))
        return jnp.repeat(jnp.exp(steps), extent[dim] // shards_of).reshape((-1,) + (1,) * (len(extent) - dim - 1))

    gain = one(*pieces[0])
    for cut in pieces[1:]:
        gain = gain * one(*cut)
    return gain


def shared_out(key, own, number, rows, amount, top, reach, skew):
    ranking = jax.random.permutation(key, amount)
    packed, usual = shares(amount, rows * top, reach, skew, True), shares(amount, rows * top, reach, skew, False)
    places = jnp.arange(amount)

    def named(lengths, offset_by):
        used = int((lengths > 0).sum())
        fixed = max(1, used // 4)
        moved = fixed + (places - fixed + offset_by * (used - fixed)) % max(1, amount - fixed)
        return jnp.zeros((amount,), jnp.int32).at[ranking[jnp.where(places < fixed, places, moved)]].set(jnp.asarray(lengths, jnp.int32))

    lengths = jnp.where(number % 4 == 0, named(packed, number // 4), named(usual, number - number // 4 - 1))
    mixed = jax.random.permutation(jax.random.fold_in(own, 3), amount)
    source_of, receiver = mixed[0:amount // 2 * 2:2], mixed[1:amount // 2 * 2:2]
    room = jnp.minimum(lengths[source_of] - 1, reach - lengths[receiver]) // 2
    room = jnp.where((source_of == ranking[0]) | (receiver == ranking[0]) | (lengths[receiver] == 0), 0, jnp.maximum(room, 0))
    moved = jax.random.randint(jax.random.fold_in(own, 4), (amount // 2,), 0, 1 << 20) % (room + 1)
    lengths = lengths.at[source_of].add(-moved).at[receiver].add(moved)
    labels = jnp.searchsorted(jnp.cumsum(lengths), jnp.arange(rows * top), side="right").astype(jnp.int32)
    table = labels.reshape(top, rows).T
    table = table[jax.random.permutation(jax.random.fold_in(own, 1), rows)]
    offset_by = jax.random.randint(jax.random.fold_in(own, 2), (rows, 1), 0, top)
    return jnp.take_along_axis(table, (jnp.arange(top)[None, :] + offset_by) % top, axis=1)


def shares(number_of, total, limit, skew, full):
    portions = [(1 << 20) // math.isqrt(standing ** skew) + 1 for standing in range(1, number_of + 1)]
    largest = limit if full else min(limit, max(-(-total // number_of), total * portions[0] // sum(portions)))
    least = 1 if total - largest >= number_of - 1 else 0
    holding, spare = [largest] + [least] * (number_of - 1), total - largest - least * (number_of - 1)
    while spare > 0:
        candidates = [i for i in range(1, number_of) if holding[i] < largest] or [i for i in range(1, number_of) if holding[i] < limit]
        pool, left = sum([portions[i] for i in candidates]), spare
        for i in candidates:
            addition = min(limit - holding[i], max(1, left * portions[i] // pool), spare)
            holding[i] = holding[i] + addition
            spare = spare - addition
    return np.array(holding)


def centred(stream_key, shape, deviation, most, shards=(), kind=jnp.bfloat16):
    array = deviation * jax.random.normal(stream_key, shape, jnp.float32)
    if shards:
        array = array * level_of(stream_key, shape, shards, -0.22, 0.18)
    return jnp.clip(array, -most, most).astype(kind)


def setup_inputs(seed: int = 0) -> dict:
    key_of = jax.random.split(jax.random.key(seed), 11)
    vel_coef = centred(key_of[0], (81, NELEM), 1.0, 6.0, ((1, 8),), jnp.float32)
    gp_block_keys = jax.random.split(jax.random.fold_in(key_of[1], 1), GP // GP_DEV)
    gp_block_turns = jax.random.permutation(jax.random.fold_in(key_of[1], 3), GP // GP_DEV)
    gp_block = jax.vmap(lambda own, number: shared_out(jax.random.fold_in(key_of[1], 2), own, number, GP_DEV, N_FLOW, 1, CAP, 2))(gp_block_keys, gp_block_turns).reshape((GP, 1))
    gp_elem = with_ends(jax.random.randint(key_of[2], (GP,), 0, E_DEV), jax.random.fold_in(key_of[2], 1), 0, E_DEV - 1).astype(jnp.int32)
    gp_param = jnp.clip(1.0 * jax.random.uniform(key_of[3], (3, GP), jnp.float32) ** level_of(key_of[3], (3, GP), ((1, 32),), -0.2, 0.2), 0.0, 1.0)
    gp_vel = centred(key_of[4], (3, GP), 1.0, 6.0, ((1, 32),), jnp.float32)
    gp_weight = jnp.clip(jnp.exp(math.log(1.0) - 2.3025851 * jax.random.uniform(key_of[5], (GP,), jnp.float32) ** level_of(key_of[5], (GP,), ((0, 32),), -0.2, 0.2)), 0.1, 1.0)
    gp_pos = centred(key_of[6], (3, GP), 0.5, 4.0, ((1, 32),), jnp.float32)
    contact_patch = with_ends(jax.random.randint(key_of[7], (GP,), 0, NP_GROUP), jax.random.fold_in(key_of[7], 1), 0, NP_GROUP - 1).astype(jnp.int32)
    contact_param = jnp.clip(1.0 * jax.random.uniform(key_of[8], (2, GP), jnp.float32) ** level_of(key_of[8], (2, GP), ((1, 32),), -0.2, 0.2), 0.0, 1.0)
    patch_ctrl = centred(key_of[9], (27, NPATCH), 0.5, 4.0, ((1, 32),), jnp.float32)
    return dict(vel_coef=vel_coef, gp_block=gp_block, gp_elem=gp_elem, gp_param=gp_param, gp_vel=gp_vel, gp_weight=gp_weight, gp_pos=gp_pos, contact_patch=contact_patch, contact_param=contact_param, patch_ctrl=patch_ctrl)


BETA = 1.5
STIFF = 2.0
REACH = 0.5


def basis(x):
    return jnp.stack([0.5 * (1.0 - x) ** 2, 0.5 * (1.0 + 2.0 * x - 2.0 * x * x), 0.5 * x * x])


def solid_weights(param):
    first, second, third = basis(param[0]), basis(param[1]), basis(param[2])
    return (first[:, None, None, :] * second[None, :, None, :] * third[None, None, :, :]).reshape(27, -1)


def shell_weights(param):
    first, second = basis(param[0]), basis(param[1])
    return (first[:, None, :] * second[None, :, :]).reshape(9, -1)


def contact_force(position, partner_coef, weights):
    near = jnp.sum(partner_coef.reshape(3, 9, -1) * weights[None], axis=1)
    gap = position - near
    return STIFF * gap / (1.0 + jnp.sum(gap * gap, axis=0) / (REACH * REACH))


def reference(vel_coef, gp_block, gp_elem, gp_param, gp_vel, gp_weight, gp_pos, contact_patch, contact_param, patch_ctrl):
    gelem = (gp_block[:, 0] * E_DEV + gp_elem).astype(jnp.int32)
    weights = solid_weights(gp_param)
    speeds = []
    for comp in range(3):
        speeds.append(jnp.sum(vel_coef[comp * 27:(comp + 1) * 27][:, gelem] * weights, axis=0))
    speed = jnp.stack(speeds)
    fsi = BETA * gp_weight[None, :] * (gp_vel - speed)
    rows = []
    for comp in range(3):
        part_rows = jnp.zeros((27, NELEM), vel_coef.dtype).at[:, gelem].add(weights * fsi[comp][None, :])
        rows.append(part_rows)
    flow_force = jnp.concatenate(rows, axis=0)
    points = jnp.arange(GP, dtype=jnp.int32)
    partner = ((points // (GP_DEV * N_LEAF)) * NP_GROUP + contact_patch).astype(jnp.int32)
    shell_w = shell_weights(contact_param)
    pushes = contact_force(gp_pos, patch_ctrl[:, partner], shell_w)
    reaction = -(pushes[:, None, :] * shell_w[None]).reshape(27, -1)
    patch_force = jnp.zeros((27, NPATCH), patch_ctrl.dtype).at[:, partner].add(reaction)
    shell_force = pushes - fsi
    return flow_force, shell_force, patch_force
```

```python
import functools

import jax
import jax.numpy as jnp
from jax import lax
from jax.experimental import pallas as pl
from jax.experimental.pallas import tpu as pltpu
from jax.sharding import PartitionSpec as P

BETA = 1.5
STIFF = 2.0
REACH = 0.5
GROUP = 512

F32, BF16, I32 = jnp.float32, jnp.bfloat16, jnp.int32
NN = (((1,), (0,)), ((), ()))
NT = (((1,), (1,)), ((), ()))


def dot(a, b, dims):
    return lax.dot_general(a, b, dims, preferred_element_type=F32)


def split(x):
    high = x.astype(BF16)
    low = (x - high.astype(F32)).astype(BF16)
    return jnp.concatenate([high, low], axis=0)


def rows_of(shape):
    return lax.broadcasted_iota(I32, shape, 0)


def one_hot(index, rows, offset=0):
    return jnp.where(rows_of((rows, index.shape[1])) == index - offset, 1.0, 0.0).astype(BF16)


def pick_basis(x, which, rows):
    b0 = 0.5 * (1.0 - x) ** 2
    b1 = 0.5 * (1.0 + 2.0 * x - 2.0 * x * x)
    b2 = 0.5 * x * x
    return jnp.where(which == 0, b0, jnp.where(which == 1, b1, b2))


def solid_weights(x0, x1, x2):
    k = rows_of((32, 1))
    return (
        pick_basis(x0, k // 9, 32)
        * pick_basis(x1, (k // 3) % 3, 32)
        * pick_basis(x2, k % 3, 32)
    )


def shell_weights(x0, x1):
    k = rows_of((16, 1))
    return pick_basis(x0, k // 3, 16) * pick_basis(x1, k % 3, 16)


def pack_kernel(block_ref, elem_ref, param_ref, vel_ref, weight_ref, out_ref, rank_ref, vals):
    owners, _, slots = out_ref.shape
    count = block_ref.shape[1]
    step = 256
    block = block_ref[...]
    mask = jnp.where(rows_of((owners, count)) == block, 1.0, 0.0)
    upto = (
        lax.broadcasted_iota(I32, (step, step), 0) <= lax.broadcasted_iota(I32, (step, step), 1)
    )
    upto = jnp.where(upto, 1.0, 0.0).astype(BF16)
    base = jnp.zeros((owners, 1), F32)
    ranks = []
    for i in range(count // step):
        part = mask[:, i * step : (i + 1) * step]
        running = dot(part.astype(BF16), upto, NN)
        ranks.append(jnp.sum(part * (running + (base - 1.0)), axis=0, keepdims=True))
        base = base + running[:, step - 1 : step]
    rank = jnp.concatenate(ranks, axis=1).astype(I32)
    rank_ref[...] = rank
    vals[0:1] = elem_ref[...].astype(F32) + 1.0
    vals[1:4] = param_ref[...]
    vals[4:7] = vel_ref[...]
    vals[7:8] = weight_ref[...]
    v = vals[...]
    terms = jnp.concatenate([v * mask[d : d + 1] for d in range(owners)], axis=0)
    packed = dot(split(terms), one_hot(rank, slots), NT)
    packed = packed[: owners * 8] + packed[owners * 8 :]
    for d in range(owners):
        out_ref[d] = packed[d * 8 : (d + 1) * 8]


def contact_kernel(me_ref, *refs, peers):
    ctrl_refs = refs[:peers]
    patch_ref, param_ref, pos_ref, coef_ref = refs[peers : peers + 4]
    push_ref, part_ref, table_ref, ctrl, wide = refs[peers + 4 :]
    own = ctrl_refs[0].shape[1]
    me = me_ref[0]
    ctrl[...] = jnp.zeros_like(ctrl)
    for k in range(peers):
        for c in range(3):
            ctrl[c * 16 : c * 16 + 9, k * own : (k + 1) * own] = ctrl_refs[k][c * 9 : c * 9 + 9, :]
    patch = patch_ref[...]
    table = jnp.concatenate([one_hot(patch, own, (me ^ k) * own) for k in range(peers)], axis=0)
    picked = dot(split(ctrl[...]), table, NN)
    picked = picked[:48] + picked[48:]
    w = shell_weights(param_ref[0:1, :], param_ref[1:2, :])
    gaps = [
        pos_ref[c : c + 1, :] - jnp.sum(picked[c * 16 : c * 16 + 16] * w, axis=0, keepdims=True)
        for c in range(3)
    ]
    far = 1.0 + (gaps[0] * gaps[0] + gaps[1] * gaps[1] + gaps[2] * gaps[2]) / (REACH * REACH)
    pushes = [STIFF * g / far for g in gaps]
    for c in range(3):
        push_ref[c : c + 1, :] = pushes[c]
    terms = jnp.concatenate([-(w * f) for f in pushes], axis=0)
    part = dot(split(terms), table, NT)
    part = part[:48] + part[48:]
    for k in range(peers):
        part_ref[k] = part[:, k * own : (k + 1) * own]
    wide[...] = jnp.zeros_like(wide)
    for c in range(3):
        wide[c * 32 : c * 32 + 27, :] = coef_ref[c * 27 : c * 27 + 27, :]
    table_ref[...] = split(wide[...])


def force_kernel(recv_ref, table_ref, part_ref, info_ref, *send_refs):
    groups = recv_ref.shape[0]
    elements = table_ref.shape[1]
    own = part_ref.shape[2]
    for g in range(groups):
        point = recv_ref[g]
        index = point[0:1].astype(I32) - 1
        picked = dot(table_ref[...], one_hot(index, elements), NN)
        picked = picked[:96] + picked[96:]
        w = solid_weights(point[1:2], point[2:3], point[3:4])
        speed = [
            jnp.sum(picked[c * 32 : c * 32 + 32] * w, axis=0, keepdims=True) for c in range(3)
        ]
        scale = BETA * point[7:8]
        info_ref[g, 0:4] = point[0:4]
        for c in range(3):
            info_ref[g, 4 + c : 5 + c] = scale * (point[4 + c : 5 + c] - speed[c])
        info_ref[g, 7:8] = jnp.zeros((1, GROUP), F32)
        for ref in send_refs:
            ref[g * 8 : (g + 1) * 8] = info_ref[g]
    for k, ref in enumerate(send_refs):
        ref[groups * 8 :, 0:own] = part_ref[k + 1, 0:24]
        ref[groups * 8 :, own:] = part_ref[k + 1, 24:48]


def spread_kernel(me_ref, info_ref, part_ref, *refs, peers):
    got_refs = refs[: peers - 1]
    flow_ref, patch_ref = refs[peers - 1 :]
    groups = info_ref.shape[0]
    rows = flow_ref.shape[1]
    own = part_ref.shape[2]
    first = me_ref[0] * rows + 1
    total = jnp.zeros((192, rows), F32)
    for k in range(peers):
        for g in range(groups):
            point = info_ref[g] if k == 0 else got_refs[k - 1][g * 8 : (g + 1) * 8]
            index = point[0:1].astype(I32)
            w = solid_weights(point[1:2], point[2:3], point[3:4])
            terms = jnp.concatenate([w * point[4 + c : 5 + c] for c in range(3)], axis=0)
            total = total + dot(split(terms), one_hot(index, rows, first), NT)
    total = total[:96] + total[96:]
    for c in range(3):
        flow_ref[c * 27 : c * 27 + 27, :] = total[c * 32 : c * 32 + 27]
    top, low = part_ref[0, 0:24], part_ref[0, 24:48]
    for ref in got_refs:
        top = top + ref[groups * 8 :, 0:own]
        low = low + ref[groups * 8 :, own:]
    both = jnp.concatenate([top, low], axis=0)
    for c in range(3):
        patch_ref[c * 9 : c * 9 + 9, :] = both[c * 16 : c * 16 + 9]


def finish_kernel(back_ref, block_ref, rank_ref, push_ref, out_ref):
    owners, _, slots = back_ref.shape
    back = back_ref[...].reshape(owners * 8, slots)
    got = dot(split(back), one_hot(rank_ref[...], slots), NN)
    got = got[: owners * 8] + got[owners * 8 :]
    block = block_ref[...]
    total = jnp.zeros((8, block.shape[1]), F32)
    for d in range(owners):
        total = total + jnp.where(block == d, got[d * 8 : (d + 1) * 8], 0.0)
    out_ref[...] = push_ref[...] - total[4:7]


def call(kernel, name, out_shape, scratch=(), smem=0, operands=(), flops=0):
    specs = [
        pl.BlockSpec(memory_space=pltpu.SMEM if i < smem else pltpu.VMEM)
        for i in range(len(operands))
    ]
    return pl.pallas_call(
        kernel,
        name=name,
        out_shape=out_shape,
        in_specs=specs,
        out_specs=jax.tree.map(lambda _: pl.BlockSpec(memory_space=pltpu.VMEM), out_shape),
        scratch_shapes=scratch,
        cost_estimate=pl.CostEstimate(flops=flops, bytes_accessed=0, transcendentals=0),
    )(*operands)


def shape(*dims, dtype=F32):
    return jax.ShapeDtypeStruct(dims, dtype)


def per_device(
    vel_coef, gp_block, gp_elem, gp_param, gp_vel, gp_weight, gp_pos, contact_patch,
    contact_param, patch_ctrl,
):
    owners = lax.axis_size("flow")
    peers = lax.axis_size("leaf")
    count = gp_elem.shape[0]
    slots = 2 * count // owners
    width = slots * owners
    groups = width // GROUP
    elements = vel_coef.shape[1]
    own = patch_ctrl.shape[1]
    me = lax.axis_index("leaf").astype(I32).reshape(1)

    def swap(x, k):
        return lax.ppermute(x, "leaf", [(i, i ^ k) for i in range(peers)])

    def to_groups(x):
        if slots == GROUP:
            return x
        return x.transpose(1, 0, 2).reshape(8, groups, GROUP).transpose(1, 0, 2)

    def to_owners(x):
        if slots == GROUP:
            return x
        return x.transpose(1, 0, 2).reshape(8, owners, slots).transpose(1, 0, 2)

    block = gp_block.reshape(1, count)
    payload, rank = call(
        pack_kernel, "pack",
        [shape(owners, 8, slots), shape(1, count, dtype=I32)],
        scratch=[pltpu.VMEM((8, count), F32)],
        operands=(block, gp_elem.reshape(1, count), gp_param, gp_vel, gp_weight.reshape(1, count)),
        flops=10**9,
    )
    recv = lax.all_to_all(payload, "flow", split_axis=0, concat_axis=0, tiled=True)
    ctrl = [patch_ctrl] + [swap(patch_ctrl, k) for k in range(1, peers)]
    pushes, part, table = call(
        functools.partial(contact_kernel, peers=peers), "contact",
        [shape(3, count), shape(peers, 48, own), shape(192, elements, dtype=BF16)],
        scratch=[pltpu.VMEM((48, peers * own), F32), pltpu.VMEM((96, elements), F32)],
        smem=1,
        operands=(me, *ctrl, contact_patch.reshape(1, count), contact_param, gp_pos, vel_coef),
        flops=10**9,
    )
    info, *sends = call(
        force_kernel, "force",
        [shape(groups, 8, GROUP)] + [shape(groups * 8 + 24, 2 * own)] * (peers - 1),
        operands=(to_groups(recv), table, part),
        flops=4 * 10**9,
    )
    gots = [swap(x, k + 1) for k, x in enumerate(sends)]
    back = lax.all_to_all(to_owners(info), "flow", split_axis=0, concat_axis=0, tiled=True)
    flow_force, patch_force = call(
        functools.partial(spread_kernel, peers=peers), "spread",
        [shape(81, elements // peers), shape(27, own)],
        smem=1,
        operands=(me, info, part, *gots),
        flops=4 * 10**9,
    )
    shell_force = call(
        finish_kernel, "finish", shape(3, count),
        operands=(back, block, rank, pushes),
        flops=10**8,
    )
    return flow_force, shell_force, patch_force


def solution(mesh):
    both = ("flow", "leaf")
    in_specs = (
        P(None, "flow"), P(both, None), P(both), P(None, both), P(None, both), P(both),
        P(None, both), P(both), P(None, both), P(None, both),
    )
    out_specs = (P(None, both), P(None, both), P(None, both))
    return jax.shard_map(
        per_device, mesh=mesh, in_specs=in_specs, out_specs=out_specs, check_vma=False
    )
```

```python
import functools

import jax
import jax.numpy as jnp
from jax import lax
from jax.experimental import pallas as pl
from jax.experimental.pallas import tpu as pltpu
from jax.sharding import PartitionSpec as P

BETA = 1.5
STIFF = 2.0
REACH = 0.5
VMEM_LIMIT = 20 * 2**20
GROUP = 512

F32, BF16, I32 = jnp.float32, jnp.bfloat16, jnp.int32
NN = (((1,), (0,)), ((), ()))
NT = (((1,), (1,)), ((), ()))


def dot(a, b, dims):
    return lax.dot_general(a, b, dims, preferred_element_type=F32)


def split(x):
    high = x.astype(BF16)
    low = (x - high.astype(F32)).astype(BF16)
    return jnp.concatenate([high, low], axis=0)


def rows_of(shape):
    return lax.broadcasted_iota(I32, shape, 0)


def one_hot(index, rows, offset=0):
    return jnp.where(rows_of((rows, index.shape[1])) == index - offset, 1.0, 0.0).astype(BF16)


def pick_basis(x, which, rows):
    b0 = 0.5 * (1.0 - x) ** 2
    b1 = 0.5 * (1.0 + 2.0 * x - 2.0 * x * x)
    b2 = 0.5 * x * x
    return jnp.where(which == 0, b0, jnp.where(which == 1, b1, b2))


def solid_weights(x0, x1, x2):
    k = rows_of((32, 1))
    return (
        pick_basis(x0, k // 9, 32)
        * pick_basis(x1, (k // 3) % 3, 32)
        * pick_basis(x2, k % 3, 32)
    )


def shell_weights(x0, x1):
    k = rows_of((16, 1))
    return pick_basis(x0, k // 3, 16) * pick_basis(x1, k % 3, 16)


def pack_kernel(block_ref, elem_ref, param_ref, vel_ref, weight_ref, out_ref, rank_ref, vals):
    owners, _, slots = out_ref.shape
    count = block_ref.shape[1]
    step = 256
    block = block_ref[...]
    mask = jnp.where(rows_of((owners, count)) == block, 1.0, 0.0)
    upto = (
        lax.broadcasted_iota(I32, (step, step), 0) <= lax.broadcasted_iota(I32, (step, step), 1)
    )
    upto = jnp.where(upto, 1.0, 0.0).astype(BF16)
    base = jnp.zeros((owners, 1), F32)
    ranks = []
    for i in range(count // step):
        part = mask[:, i * step : (i + 1) * step]
        running = dot(part.astype(BF16), upto, NN)
        ranks.append(jnp.sum(part * (running + (base - 1.0)), axis=0, keepdims=True))
        base = base + running[:, step - 1 : step]
    rank = jnp.concatenate(ranks, axis=1).astype(I32)
    rank_ref[...] = rank
    vals[0:1] = elem_ref[...].astype(F32) + 1.0
    vals[1:4] = param_ref[...]
    vals[4:7] = vel_ref[...]
    vals[7:8] = weight_ref[...]
    v = vals[...]
    terms = jnp.concatenate([v * mask[d : d + 1] for d in range(owners)], axis=0)
    packed = dot(split(terms), one_hot(rank, slots), NT)
    packed = packed[: owners * 8] + packed[owners * 8 :]
    for d in range(owners):
        out_ref[d] = packed[d * 8 : (d + 1) * 8]


def contact_kernel(me_ref, *refs, peers):
    ctrl_refs = refs[:peers]
    patch_ref, param_ref, pos_ref, coef_ref = refs[peers : peers + 4]
    push_ref, keep_ref, give_ref, table_ref, ctrl, wide = refs[peers + 4 :]
    own = ctrl_refs[0].shape[1]
    me = me_ref[0]
    ctrl[...] = jnp.zeros_like(ctrl)
    for k in range(peers):
        for c in range(3):
            ctrl[c * 16 : c * 16 + 9, k * own : (k + 1) * own] = ctrl_refs[k][c * 9 : c * 9 + 9, :]
    patch = patch_ref[...]
    table = jnp.concatenate([one_hot(patch, own, (me ^ k) * own) for k in range(peers)], axis=0)
    picked = dot(split(ctrl[...]), table, NN)
    picked = picked[:48] + picked[48:]
    w = shell_weights(param_ref[0:1, :], param_ref[1:2, :])
    gaps = [
        pos_ref[c : c + 1, :] - jnp.sum(picked[c * 16 : c * 16 + 16] * w, axis=0, keepdims=True)
        for c in range(3)
    ]
    far = 1.0 + (gaps[0] * gaps[0] + gaps[1] * gaps[1] + gaps[2] * gaps[2]) / (REACH * REACH)
    pushes = [STIFF * g / far for g in gaps]
    for c in range(3):
        push_ref[c : c + 1, :] = pushes[c]
    terms = jnp.concatenate([-(w * f) for f in pushes], axis=0)
    part = dot(split(terms), table, NT)
    part = part[:48] + part[48:]
    for k in range(peers):
        ref = give_ref if k % 2 else keep_ref
        ref[k // 2] = part[:, k * own : (k + 1) * own]
    wide[...] = jnp.zeros_like(wide)
    for c in range(3):
        wide[c * 32 : c * 32 + 27, :] = coef_ref[c * 27 : c * 27 + 27, :]
    table_ref[...] = split(wide[...])


def force_kernel(recv_ref, table_ref, keep_ref, gave_ref, info_ref, send_ref, patch_ref):
    groups = recv_ref.shape[0]
    elements = table_ref.shape[1]
    own = keep_ref.shape[2]
    for g in range(groups):
        point = recv_ref[g]
        index = point[0:1].astype(I32) - 1
        picked = dot(table_ref[...], one_hot(index, elements), NN)
        picked = picked[:96] + picked[96:]
        w = solid_weights(point[1:2], point[2:3], point[3:4])
        speed = [
            jnp.sum(picked[c * 32 : c * 32 + 32] * w, axis=0, keepdims=True) for c in range(3)
        ]
        scale = BETA * point[7:8]
        info_ref[g, 0:4] = point[0:4]
        for c in range(3):
            info_ref[g, 4 + c : 5 + c] = scale * (point[4 + c : 5 + c] - speed[c])
        info_ref[g, 7:8] = jnp.zeros((1, GROUP), F32)
        send_ref[g * 8 : (g + 1) * 8] = info_ref[g]
    patch_ref[...] = keep_ref[0] + gave_ref[0]
    across = keep_ref[1] + gave_ref[1]
    send_ref[groups * 8 :, 0:own] = across[0:24]
    send_ref[groups * 8 :, own:] = across[24:48]


def spread(source_ref, terms, first, rows):
    groups = terms.shape[1] // GROUP
    index = []
    for g in range(groups):
        point = source_ref[g * 8 : (g + 1) * 8]
        index.append(point[0:1].astype(I32))
        w = solid_weights(point[1:2], point[2:3], point[3:4])
        part = jnp.concatenate([w * point[4 + c : 5 + c] for c in range(3)], axis=0)
        terms[:, g * GROUP : (g + 1) * GROUP] = split(part)
    return dot(terms[...], one_hot(jnp.concatenate(index, axis=1), rows, first), NT)


def near_kernel(me_ref, *refs):
    *sources, part_ref, total_ref, patch_ref, terms = refs
    rows = total_ref.shape[1]
    own = part_ref.shape[1]
    first = me_ref[0] * rows + 1
    total = spread(sources[0], terms, first, rows)
    for source in sources[1:]:
        total = total + spread(source, terms, first, rows)
    total_ref[...] = total[:96] + total[96:]
    skip = sources[-1].shape[0] - 24
    top = part_ref[0:24] + sources[-1][skip:, 0:own]
    low = part_ref[24:48] + sources[-1][skip:, own:]
    both = jnp.concatenate([top, low], axis=0)
    for c in range(3):
        patch_ref[c * 9 : c * 9 + 9, :] = both[c * 16 : c * 16 + 9]


def last_kernel(me_ref, source_ref, total_ref, flow_ref, terms):
    rows = total_ref.shape[1]
    total = spread(source_ref, terms, me_ref[0] * rows + 1, rows)
    total = total_ref[...] + total[:96] + total[96:]
    for c in range(3):
        flow_ref[c * 27 : c * 27 + 27, :] = total[c * 32 : c * 32 + 27]


def finish_kernel(back_ref, block_ref, rank_ref, push_ref, out_ref):
    owners, _, slots = back_ref.shape
    back = back_ref[...].reshape(owners * 8, slots)
    got = dot(split(back), one_hot(rank_ref[...], slots), NN)
    got = got[: owners * 8] + got[owners * 8 :]
    block = block_ref[...]
    total = jnp.zeros((8, block.shape[1]), F32)
    for d in range(owners):
        total = total + jnp.where(block == d, got[d * 8 : (d + 1) * 8], 0.0)
    out_ref[...] = push_ref[...] - total[4:7]


def call(kernel, name, out_shape, scratch=(), smem=0, operands=(), flops=0, limit=VMEM_LIMIT):
    specs = [
        pl.BlockSpec(memory_space=pltpu.SMEM if i < smem else pltpu.VMEM)
        for i in range(len(operands))
    ]
    return pl.pallas_call(
        kernel,
        name=name,
        out_shape=out_shape,
        in_specs=specs,
        out_specs=jax.tree.map(lambda _: pl.BlockSpec(memory_space=pltpu.VMEM), out_shape),
        scratch_shapes=scratch,
        cost_estimate=pl.CostEstimate(flops=flops, bytes_accessed=0, transcendentals=0),
        compiler_params=pltpu.CompilerParams(vmem_limit_bytes=limit),
    )(*operands)


def shape(*dims, dtype=F32):
    return jax.ShapeDtypeStruct(dims, dtype)


def per_device(
    vel_coef, gp_block, gp_elem, gp_param, gp_vel, gp_weight, gp_pos, contact_patch,
    contact_param, patch_ctrl,
):
    owners = lax.axis_size("flow")
    peers = lax.axis_size("leaf")
    count = gp_elem.shape[0]
    slots = 2 * count // owners
    width = slots * owners
    groups = width // GROUP
    elements = vel_coef.shape[1]
    own = patch_ctrl.shape[1]
    me = lax.axis_index("leaf").astype(I32).reshape(1)

    def swap(x, k):
        return lax.ppermute(x, "leaf", [(i, i ^ k) for i in range(peers)])

    def to_groups(x):
        if slots == GROUP:
            return x
        return x.transpose(1, 0, 2).reshape(8, groups, GROUP).transpose(1, 0, 2)

    def to_owners(x):
        if slots == GROUP:
            return x
        return x.transpose(1, 0, 2).reshape(8, owners, slots).transpose(1, 0, 2)

    block = gp_block.reshape(1, count)
    ctrl = [patch_ctrl, swap(patch_ctrl, 1), swap(patch_ctrl, 2)]
    payload, rank = call(
        pack_kernel, "pack",
        [shape(owners, 8, slots), shape(1, count, dtype=I32)],
        scratch=[pltpu.VMEM((8, count), F32)],
        operands=(block, gp_elem.reshape(1, count), gp_param, gp_vel, gp_weight.reshape(1, count)),
        flops=10**9,
        limit=None,
    )
    payload, *ctrl = lax.optimization_barrier((payload, *ctrl))
    ctrl.append(swap(ctrl[2], 1))
    recv = lax.all_to_all(payload, "flow", split_axis=0, concat_axis=0, tiled=True)
    pushes, keep, give, table = call(
        functools.partial(contact_kernel, peers=peers), "contact",
        [
            shape(3, count), shape(2, 48, own), shape(2, 48, own),
            shape(192, elements, dtype=BF16),
        ],
        scratch=[pltpu.VMEM((48, peers * own), F32), pltpu.VMEM((96, elements), F32)],
        smem=1,
        operands=(me, *ctrl, contact_patch.reshape(1, count), contact_param, gp_pos, vel_coef),
        flops=10**9,
    )
    gave = swap(give, 1)
    info, send, patch_part = call(
        force_kernel, "force",
        [shape(groups, 8, GROUP), shape(groups * 8 + 24, 2 * own), shape(48, own)],
        operands=(to_groups(recv), table, keep, gave),
        flops=4 * 10**9,
    )
    across = swap(send, 2)
    beside = swap(send, 1)
    back = lax.all_to_all(to_owners(info), "flow", split_axis=0, concat_axis=0, tiled=True)
    corner = swap(across, 1)
    rows = elements // peers
    total, patch_force = call(
        near_kernel, "near",
        [shape(96, rows), shape(27, own)],
        scratch=[pltpu.VMEM((192, width), BF16)],
        smem=1,
        operands=(me, send, beside, across, patch_part),
        flops=3 * 10**9,
    )
    flow_force = call(
        last_kernel, "last", shape(81, rows),
        scratch=[pltpu.VMEM((192, width), BF16)],
        smem=1,
        operands=(me, corner, total),
        flops=10**9,
    )
    shell_force = call(
        finish_kernel, "finish", shape(3, count),
        operands=(back, block, rank, pushes),
        flops=10**8,
    )
    return flow_force, shell_force, patch_force


def solution(mesh):
    both = ("flow", "leaf")
    in_specs = (
        P(None, "flow"), P(both, None), P(both), P(None, both), P(None, both), P(both),
        P(None, both), P(both), P(None, both), P(None, both),
    )
    out_specs = (P(None, both), P(None, both), P(None, both))
    return jax.shard_map(
        per_device, mesh=mesh, in_specs=in_specs, out_specs=out_specs, check_vma=False
    )
```

```python
import functools

import jax
import jax.numpy as jnp
from jax import lax
from jax.experimental import pallas as pl
from jax.experimental.pallas import tpu as pltpu
from jax.sharding import PartitionSpec as P


BETA = 1.5
STIFF = 2.0
REACH = 0.5
VMEM_LIMIT = 20 * 2**20
GROUP = 512

F32, BF16, F8 = jnp.float32, jnp.bfloat16, jnp.float8_e4m3fn
I32, I16 = jnp.int32, jnp.int16
NN = (((1,), (0,)), ((), ()))
NT = (((1,), (1,)), ((), ()))


def dot(a, b, dims):
    return lax.dot_general(a, b, dims, preferred_element_type=F32)


def split(x):
    high = x.astype(BF16)
    low = (x - high.astype(F32)).astype(BF16)
    return jnp.concatenate([high, low], axis=0)


def rows_of(shape):
    return lax.broadcasted_iota(I32, shape, 0)


def one_hot(index, rows, offset=0):
    number = lax.broadcasted_iota(I16, (rows, index.shape[1]), 0)
    hit = number == (index - offset).astype(I16)
    return jnp.where(hit, jnp.asarray(1, BF16), jnp.asarray(0, BF16)).astype(F8)


def pick_basis(x, which):
    b0 = 0.5 * (1.0 - x) ** 2
    b1 = 0.5 * (1.0 + 2.0 * x - 2.0 * x * x)
    b2 = 0.5 * x * x
    return jnp.where(which == 0, b0, jnp.where(which == 1, b1, b2))


def solid_weights(x0, x1, x2):
    k = rows_of((32, 1))
    return pick_basis(x0, k // 9) * pick_basis(x1, (k // 3) % 3) * pick_basis(x2, k % 3)


def shell_weights(x0, x1):
    k = rows_of((16, 1))
    return pick_basis(x0, k // 3) * pick_basis(x1, k % 3)


def pack_kernel(block_ref, elem_ref, param_ref, vel_ref, weight_ref, out_ref, rank_ref, vals):
    owners, _, slots = out_ref.shape
    count = block_ref.shape[1]
    step = 256
    block = block_ref[...]
    mask = jnp.where(rows_of((owners, count)) == block, 1.0, 0.0)
    upto = (
        lax.broadcasted_iota(I32, (step, step), 0) <= lax.broadcasted_iota(I32, (step, step), 1)
    )
    upto = jnp.where(upto, 1.0, 0.0).astype(BF16)
    base = jnp.zeros((owners, 1), F32)
    ranks = []
    for i in range(count // step):
        part = mask[:, i * step : (i + 1) * step]
        running = dot(part.astype(BF16), upto, NN)
        ranks.append(jnp.sum(part * (running + (base - 1.0)), axis=0, keepdims=True))
        base = base + running[:, step - 1 : step]
    rank = jnp.concatenate(ranks, axis=1).astype(I32)
    rank_ref[...] = rank
    vals[0:1] = elem_ref[...].astype(F32) + 1.0
    vals[1:4] = param_ref[...]
    vals[4:7] = vel_ref[...]
    vals[7:8] = weight_ref[...]
    v = vals[...]
    terms = jnp.concatenate([v * mask[d : d + 1] for d in range(owners)], axis=0)
    packed = dot(split(terms), one_hot(rank, slots), NT)
    packed = packed[: owners * 8] + packed[owners * 8 :]
    for d in range(owners):
        out_ref[d] = packed[d * 8 : (d + 1) * 8]


def contact_kernel(me_ref, *refs, peers):
    ctrl_refs = refs[:peers]
    patch_ref, param_ref, pos_ref, coef_ref = refs[peers : peers + 4]
    push_ref, part_ref, table_ref, ctrl, tight, wide = refs[peers + 4 :]
    own = ctrl_refs[0].shape[1]
    me = me_ref[0]
    ctrl[...] = jnp.zeros_like(ctrl)
    for k in range(peers):
        for c in range(3):
            ctrl[c * 16 : c * 16 + 9, k * own : (k + 1) * own] = ctrl_refs[k][c * 9 : c * 9 + 9, :]
    patch = patch_ref[...]
    table = jnp.concatenate([one_hot(patch, own, (me ^ k) * own) for k in range(peers)], axis=0)
    picked = dot(split(ctrl[...]), table, NN)
    picked = picked[:48] + picked[48:]
    w = shell_weights(param_ref[0:1, :], param_ref[1:2, :])
    gaps = [
        pos_ref[c : c + 1, :] - jnp.sum(picked[c * 16 : c * 16 + 16] * w, axis=0, keepdims=True)
        for c in range(3)
    ]
    far = 1.0 + (gaps[0] * gaps[0] + gaps[1] * gaps[1] + gaps[2] * gaps[2]) / (REACH * REACH)
    pushes = [STIFF * g / far for g in gaps]
    for c in range(3):
        push_ref[c : c + 1, :] = pushes[c]
    terms = jnp.concatenate([-(w * f) for f in pushes], axis=0)
    part = dot(split(terms), table, NT)
    part = part[:48] + part[48:]
    for c in range(3):
        tight[c * 9 : c * 9 + 9] = part[c * 16 : c * 16 + 9]
    part_ref[...] = jnp.zeros_like(part_ref)
    for k in range(peers):
        part_ref[k, 0:14, 0:own] = tight[0:14, k * own : (k + 1) * own]
        part_ref[k, 0:13, own:] = tight[14:27, k * own : (k + 1) * own]
    wide[...] = jnp.zeros_like(wide)
    for c in range(3):
        wide[c * 32 : c * 32 + 27, :] = coef_ref[c * 27 : c * 27 + 27, :]
    table_ref[...] = split(wide[...])


def force_kernel(recv_ref, table_ref, part_ref, info_ref, beside_ref, across_ref):
    groups = recv_ref.shape[0]
    elements = table_ref.shape[1]
    for g in range(groups):
        point = recv_ref[g]
        index = point[0:1].astype(I32) - 1
        picked = dot(table_ref[...], one_hot(index, elements), NN)
        picked = picked[:96] + picked[96:]
        w = solid_weights(point[1:2], point[2:3], point[3:4])
        speed = [
            jnp.sum(picked[c * 32 : c * 32 + 32] * w, axis=0, keepdims=True) for c in range(3)
        ]
        scale = BETA * point[7:8]
        info_ref[g, 0:4] = point[0:4]
        for c in range(3):
            info_ref[g, 4 + c : 5 + c] = scale * (point[4 + c : 5 + c] - speed[c])
        info_ref[g, 7:8] = jnp.zeros((1, GROUP), F32)
        beside_ref[g * 8 : (g + 1) * 8] = info_ref[g]
        across_ref[g * 8 : (g + 1) * 8] = info_ref[g]
    tail = groups * 8
    beside_ref[tail:] = part_ref[1]
    across_ref[tail : tail + 16] = part_ref[2]
    across_ref[tail + 16 :] = part_ref[3]


def spread(source_ref, terms, first, rows):
    groups = terms.shape[1] // GROUP
    index = []
    for g in range(groups):
        point = source_ref[g * 8 : (g + 1) * 8]
        index.append(point[0:1].astype(I32))
        w = solid_weights(point[1:2], point[2:3], point[3:4])
        part = jnp.concatenate([w * point[4 + c : 5 + c] for c in range(3)], axis=0)
        terms[:, g * GROUP : (g + 1) * GROUP] = split(part)
    return dot(terms[...], one_hot(jnp.concatenate(index, axis=1), rows, first), NT)


def near_kernel(me_ref, own_ref, across_ref, part_ref, total_ref, patch_ref, terms):
    rows = total_ref.shape[1]
    tail = terms.shape[1] // GROUP * 8
    first = me_ref[0] * rows + 1
    total = spread(own_ref, terms, first, rows)
    total = total + spread(across_ref, terms, first, rows)
    total_ref[...] = total[:96] + total[96:]
    patch_ref[...] = part_ref[0] + across_ref[tail : tail + 16]


def last_kernel(me_ref, beside_ref, corner_ref, total_ref, part_ref, flow_ref, patch_ref, terms):
    rows = total_ref.shape[1]
    own = patch_ref.shape[1]
    tail = terms.shape[1] // GROUP * 8
    first = me_ref[0] * rows + 1
    total = spread(beside_ref, terms, first, rows)
    total = total + spread(corner_ref, terms, first, rows)
    total = total_ref[...] + total[:96] + total[96:]
    for c in range(3):
        flow_ref[c * 27 : c * 27 + 27, :] = total[c * 32 : c * 32 + 27]
    part = part_ref[...] + beside_ref[tail:] + corner_ref[tail + 16 :]
    patch_ref[0:14] = part[0:14, 0:own]
    patch_ref[14:27] = part[0:13, own:]


def finish_kernel(back_ref, block_ref, rank_ref, push_ref, out_ref):
    owners, _, slots = back_ref.shape
    back = back_ref[...].reshape(owners * 8, slots)
    got = dot(split(back), one_hot(rank_ref[...], slots), NN)
    got = got[: owners * 8] + got[owners * 8 :]
    block = block_ref[...]
    total = jnp.zeros((8, block.shape[1]), F32)
    for d in range(owners):
        total = total + jnp.where(block == d, got[d * 8 : (d + 1) * 8], 0.0)
    out_ref[...] = push_ref[...] - total[4:7]


def call(kernel, out_shape, scratch=(), smem=0, operands=(), flops=0, limit=VMEM_LIMIT):
    specs = [
        pl.BlockSpec(memory_space=pltpu.SMEM if i < smem else pltpu.VMEM)
        for i in range(len(operands))
    ]
    return pl.pallas_call(
        kernel,
        out_shape=out_shape,
        in_specs=specs,
        out_specs=jax.tree.map(lambda _: pl.BlockSpec(memory_space=pltpu.VMEM), out_shape),
        scratch_shapes=scratch,
        cost_estimate=pl.CostEstimate(flops=flops, bytes_accessed=0, transcendentals=0),
        compiler_params=pltpu.CompilerParams(vmem_limit_bytes=limit),
    )(*operands)


def shape(*dims, dtype=F32):
    return jax.ShapeDtypeStruct(dims, dtype)


def per_device(
    vel_coef, gp_block, gp_elem, gp_param, gp_vel, gp_weight, gp_pos, contact_patch,
    contact_param, patch_ctrl,
):
    owners = lax.axis_size("flow")
    peers = lax.axis_size("leaf")
    count = gp_elem.shape[0]
    slots = 2 * count // owners
    width = slots * owners
    groups = width // GROUP
    elements = vel_coef.shape[1]
    own = patch_ctrl.shape[1]
    me = lax.axis_index("leaf").astype(I32).reshape(1)

    def swap(x, k):
        return lax.ppermute(x, "leaf", [(i, i ^ k) for i in range(peers)])

    def to_groups(x):
        if slots == GROUP:
            return x
        return x.transpose(1, 0, 2).reshape(8, groups, GROUP).transpose(1, 0, 2)

    def to_owners(x):
        if slots == GROUP:
            return x
        return x.transpose(1, 0, 2).reshape(8, owners, slots).transpose(1, 0, 2)

    block = gp_block.reshape(1, count)
    far = swap(patch_ctrl, 2)
    payload, rank = call(
        pack_kernel,
        [shape(owners, 8, slots), shape(1, count, dtype=I32)],
        scratch=[pltpu.VMEM((8, count), F32)],
        operands=(block, gp_elem.reshape(1, count), gp_param, gp_vel, gp_weight.reshape(1, count)),
        flops=10**9,
        limit=None,
    )
    payload, far, here = lax.optimization_barrier((payload, far, patch_ctrl))
    ctrl = [here, swap(here, 1), far, swap(far, 1)]
    recv = lax.all_to_all(payload, "flow", split_axis=0, concat_axis=0, tiled=True)
    pushes, part, table = call(
        functools.partial(contact_kernel, peers=peers),
        [shape(3, count), shape(peers, 16, 2 * own), shape(192, elements, dtype=BF16)],
        scratch=[
            pltpu.VMEM((48, peers * own), F32),
            pltpu.VMEM((32, peers * own), F32),
            pltpu.VMEM((96, elements), F32),
        ],
        smem=1,
        operands=(me, *ctrl, contact_patch.reshape(1, count), contact_param, gp_pos, vel_coef),
        flops=10**9,
    )
    tail = groups * 8
    info, beside, across = call(
        force_kernel,
        [shape(groups, 8, GROUP), shape(tail + 16, GROUP), shape(tail + 32, GROUP)],
        operands=(to_groups(recv), table, part),
        flops=4 * 10**9,
    )
    from_across = swap(across, 2)
    back = lax.all_to_all(to_owners(info), "flow", split_axis=0, concat_axis=0, tiled=True)
    from_corner = swap(from_across, 1)
    from_beside = swap(beside, 1)
    rows = elements // peers
    total, patch_part = call(
        near_kernel,
        [shape(96, rows), shape(16, 2 * own)],
        scratch=[pltpu.VMEM((192, width), BF16)],
        smem=1,
        operands=(me, beside, from_across, part),
        flops=2 * 10**9,
    )
    flow_force, patch_force = call(
        last_kernel,
        [shape(81, rows), shape(27, own)],
        scratch=[pltpu.VMEM((192, width), BF16)],
        smem=1,
        operands=(me, from_beside, from_corner, total, patch_part),
        flops=2 * 10**9,
    )
    flow_force, pushes = lax.optimization_barrier((flow_force, pushes))
    shell_force = call(
        finish_kernel, shape(3, count),
        operands=(back, block, rank, pushes),
        flops=10**8,
    )
    return flow_force, shell_force, patch_force


def solution(mesh):
    both = ("flow", "leaf")
    in_specs = (
        P(None, "flow"), P(both, None), P(both), P(None, both), P(None, both), P(both),
        P(None, both), P(both), P(None, both), P(None, both),
    )
    out_specs = (P(None, both), P(None, both), P(None, both))

    return jax.shard_map(
        per_device, mesh=mesh, in_specs=in_specs, out_specs=out_specs, check_vma=False
    )
```

```python
import functools

import jax
import jax.numpy as jnp
from jax import lax
from jax.experimental import pallas as pl
from jax.experimental.pallas import tpu as pltpu
from jax.sharding import PartitionSpec as P


BETA = 1.5
STIFF = 2.0
REACH = 0.5
VMEM_LIMIT = 20 * 2**20
GROUP = 512

F32, BF16, F8 = jnp.float32, jnp.bfloat16, jnp.float8_e4m3fn
I32, I16 = jnp.int32, jnp.int16
NN = (((1,), (0,)), ((), ()))
NT = (((1,), (1,)), ((), ()))


def dot(a, b, dims):
    return lax.dot_general(a, b, dims, preferred_element_type=F32)


def split(x):
    high = x.astype(BF16)
    low = (x - high.astype(F32)).astype(BF16)
    return jnp.concatenate([high, low], axis=0)


def rows_of(shape):
    return lax.broadcasted_iota(I32, shape, 0)


def one_hot(index, rows, offset=0):
    number = lax.broadcasted_iota(I16, (rows, index.shape[1]), 0)
    hit = number == (index - offset).astype(I16)
    return jnp.where(hit, jnp.asarray(1, BF16), jnp.asarray(0, BF16)).astype(F8)


def pick_basis(x, which):
    b0 = 0.5 * (1.0 - x) ** 2
    b1 = 0.5 * (1.0 + 2.0 * x - 2.0 * x * x)
    b2 = 0.5 * x * x
    return jnp.where(which == 0, b0, jnp.where(which == 1, b1, b2))


def solid_weights(x0, x1, x2):
    k = rows_of((32, 1))
    return pick_basis(x0, k // 9) * pick_basis(x1, (k // 3) % 3) * pick_basis(x2, k % 3)


def shell_weights(x0, x1):
    k = rows_of((16, 1))
    return pick_basis(x0, k // 3) * pick_basis(x1, k % 3)


def pack_kernel(block_ref, elem_ref, param_ref, vel_ref, weight_ref, out_ref, rank_ref, vals):
    owners, _, slots = out_ref.shape
    count = block_ref.shape[1]
    step = 256
    block = block_ref[...]
    mask = jnp.where(rows_of((owners, count)) == block, 1.0, 0.0)
    upto = (
        lax.broadcasted_iota(I32, (step, step), 0) <= lax.broadcasted_iota(I32, (step, step), 1)
    )
    upto = jnp.where(upto, 1.0, 0.0).astype(BF16)
    base = jnp.zeros((owners, 1), F32)
    ranks = []
    for i in range(count // step):
        part = mask[:, i * step : (i + 1) * step]
        running = dot(part.astype(BF16), upto, NN)
        ranks.append(jnp.sum(part * (running + (base - 1.0)), axis=0, keepdims=True))
        base = base + running[:, step - 1 : step]
    rank = jnp.concatenate(ranks, axis=1).astype(I32)
    rank_ref[...] = rank
    vals[0:1] = elem_ref[...].astype(F32) + 1.0
    vals[1:4] = param_ref[...]
    vals[4:7] = vel_ref[...]
    vals[7:8] = weight_ref[...]
    v = vals[...]
    terms = jnp.concatenate([v * mask[d : d + 1] for d in range(owners)], axis=0)
    packed = dot(split(terms), one_hot(rank, slots), NT)
    packed = packed[: owners * 8] + packed[owners * 8 :]
    for d in range(owners):
        out_ref[d] = packed[d * 8 : (d + 1) * 8]


def contact_kernel(me_ref, *refs, peers):
    ctrl_refs = refs[:peers]
    patch_ref, param_ref, pos_ref, coef_ref = refs[peers : peers + 4]
    push_ref, part_ref, table_ref, ctrl, tight, wide = refs[peers + 4 :]
    own = ctrl_refs[0].shape[1]
    me = me_ref[0]
    ctrl[...] = jnp.zeros_like(ctrl)
    for k in range(peers):
        for c in range(3):
            ctrl[c * 16 : c * 16 + 9, k * own : (k + 1) * own] = ctrl_refs[k][c * 9 : c * 9 + 9, :]
    patch = patch_ref[...]
    table = jnp.concatenate([one_hot(patch, own, (me ^ k) * own) for k in range(peers)], axis=0)
    picked = dot(split(ctrl[...]), table, NN)
    picked = picked[:48] + picked[48:]
    w = shell_weights(param_ref[0:1, :], param_ref[1:2, :])
    gaps = [
        pos_ref[c : c + 1, :] - jnp.sum(picked[c * 16 : c * 16 + 16] * w, axis=0, keepdims=True)
        for c in range(3)
    ]
    far = 1.0 + (gaps[0] * gaps[0] + gaps[1] * gaps[1] + gaps[2] * gaps[2]) / (REACH * REACH)
    pushes = [STIFF * g / far for g in gaps]
    for c in range(3):
        push_ref[c : c + 1, :] = pushes[c]
    terms = jnp.concatenate([-(w * f) for f in pushes], axis=0)
    part = dot(split(terms), table, NT)
    part = part[:48] + part[48:]
    for c in range(3):
        tight[c * 9 : c * 9 + 9] = part[c * 16 : c * 16 + 9]
    part_ref[...] = jnp.zeros_like(part_ref)
    for k in range(peers):
        part_ref[k, 0:14, 0:own] = tight[0:14, k * own : (k + 1) * own]
        part_ref[k, 0:13, own:] = tight[14:27, k * own : (k + 1) * own]
    wide[...] = jnp.zeros_like(wide)
    for c in range(3):
        wide[c * 32 : c * 32 + 27, :] = coef_ref[c * 27 : c * 27 + 27, :]
    table_ref[...] = split(wide[...])


def force_kernel(recv_ref, table_ref, part_ref, back_ref, beside_ref, across_ref):
    groups = recv_ref.shape[0]
    elements = table_ref.shape[1]
    for g in range(groups):
        point = recv_ref[g]
        index = point[0:1].astype(I32) - 1
        picked = dot(table_ref[...], one_hot(index, elements), NN)
        picked = picked[:96] + picked[96:]
        w = solid_weights(point[1:2], point[2:3], point[3:4])
        speed = [
            jnp.sum(picked[c * 32 : c * 32 + 32] * w, axis=0, keepdims=True) for c in range(3)
        ]
        scale = BETA * point[7:8]
        beside_ref[g * 8 : g * 8 + 4] = point[0:4]
        for c in range(3):
            force = scale * (point[4 + c : 5 + c] - speed[c])
            beside_ref[g * 8 + 4 + c : g * 8 + 5 + c] = force
            back_ref[g, c : c + 1] = force
        beside_ref[g * 8 + 7 : g * 8 + 8] = jnp.zeros((1, GROUP), F32)
        back_ref[g, 3:4] = jnp.zeros((1, GROUP), F32)
        across_ref[g * 8 : (g + 1) * 8] = beside_ref[g * 8 : (g + 1) * 8]
    tail = groups * 8
    beside_ref[tail:] = part_ref[1]
    across_ref[tail : tail + 16] = part_ref[2]
    across_ref[tail + 16 :] = part_ref[3]


def spread(source_ref, terms, first, rows):
    groups = terms.shape[1] // GROUP
    index = []
    for g in range(groups):
        point = source_ref[g * 8 : (g + 1) * 8]
        index.append(point[0:1].astype(I32))
        w = solid_weights(point[1:2], point[2:3], point[3:4])
        part = jnp.concatenate([w * point[4 + c : 5 + c] for c in range(3)], axis=0)
        terms[:, g * GROUP : (g + 1) * GROUP] = split(part)
    return dot(terms[...], one_hot(jnp.concatenate(index, axis=1), rows, first), NT)


def near_kernel(me_ref, own_ref, across_ref, part_ref, total_ref, patch_ref, terms):
    rows = total_ref.shape[1]
    tail = terms.shape[1] // GROUP * 8
    first = me_ref[0] * rows + 1
    total = spread(own_ref, terms, first, rows)
    total = total + spread(across_ref, terms, first, rows)
    total_ref[...] = total[:96] + total[96:]
    patch_ref[...] = part_ref[0] + across_ref[tail : tail + 16]


def last_kernel(me_ref, beside_ref, corner_ref, total_ref, part_ref, flow_ref, patch_ref, terms):
    rows = total_ref.shape[1]
    own = patch_ref.shape[1]
    tail = terms.shape[1] // GROUP * 8
    first = me_ref[0] * rows + 1
    total = spread(beside_ref, terms, first, rows)
    total = total + spread(corner_ref, terms, first, rows)
    total = total_ref[...] + total[:96] + total[96:]
    for c in range(3):
        flow_ref[c * 27 : c * 27 + 27, :] = total[c * 32 : c * 32 + 27]
    part = part_ref[...] + beside_ref[tail:] + corner_ref[tail + 16 :]
    patch_ref[0:14] = part[0:14, 0:own]
    patch_ref[14:27] = part[0:13, own:]


def finish_kernel(back_ref, block_ref, rank_ref, push_ref, out_ref, rows):
    owners, _, slots = back_ref.shape
    for d in range(owners):
        rows[d * 4 : (d + 1) * 4] = back_ref[d]
    got = dot(split(rows[...]), one_hot(rank_ref[...], slots), NN)
    got = got[: owners * 4] + got[owners * 4 :]
    block = block_ref[...]
    half = rows_of((8, 1)) // 4
    total = jnp.zeros((8, block.shape[1]), F32)
    for d in range(owners // 2):
        total = total + jnp.where(block - half == 2 * d, got[d * 8 : (d + 1) * 8], 0.0)
    out_ref[...] = push_ref[...] - (total[0:3] + total[4:7])


def call(kernel, out_shape, scratch=(), smem=0, operands=(), flops=0, limit=VMEM_LIMIT):
    specs = [
        pl.BlockSpec(memory_space=pltpu.SMEM if i < smem else pltpu.VMEM)
        for i in range(len(operands))
    ]
    return pl.pallas_call(
        kernel,
        out_shape=out_shape,
        in_specs=specs,
        out_specs=jax.tree.map(lambda _: pl.BlockSpec(memory_space=pltpu.VMEM), out_shape),
        scratch_shapes=scratch,
        cost_estimate=pl.CostEstimate(flops=flops, bytes_accessed=0, transcendentals=0),
        compiler_params=pltpu.CompilerParams(vmem_limit_bytes=limit),
    )(*operands)


def shape(*dims, dtype=F32):
    return jax.ShapeDtypeStruct(dims, dtype)


def per_device(
    vel_coef, gp_block, gp_elem, gp_param, gp_vel, gp_weight, gp_pos, contact_patch,
    contact_param, patch_ctrl,
):
    owners = lax.axis_size("flow")
    peers = lax.axis_size("leaf")
    count = gp_elem.shape[0]
    slots = 2 * count // owners
    width = slots * owners
    groups = width // GROUP
    elements = vel_coef.shape[1]
    own = patch_ctrl.shape[1]
    me = lax.axis_index("leaf").astype(I32).reshape(1)

    def swap(x, k):
        return lax.ppermute(x, "leaf", [(i, i ^ k) for i in range(peers)])

    def to_groups(x):
        if slots == GROUP:
            return x
        return x.transpose(1, 0, 2).reshape(-1, groups, GROUP).transpose(1, 0, 2)

    def to_owners(x):
        if slots == GROUP:
            return x
        return x.transpose(1, 0, 2).reshape(-1, owners, slots).transpose(1, 0, 2)

    block = gp_block.reshape(1, count)
    payload, rank = call(
        pack_kernel,
        [shape(owners, 8, slots), shape(1, count, dtype=I32)],
        scratch=[pltpu.VMEM((8, count), F32)],
        operands=(block, gp_elem.reshape(1, count), gp_param, gp_vel, gp_weight.reshape(1, count)),
        flops=10**9,
        limit=None,
    )
    payload, here = lax.optimization_barrier((payload, patch_ctrl))
    far = swap(here, 2)
    recv = lax.all_to_all(payload, "flow", split_axis=0, concat_axis=0, tiled=True)
    twin = swap(here, 1)
    diag = swap(far, 1)
    ctrl = (here, twin, far, diag)
    pushes, part, table = call(
        functools.partial(contact_kernel, peers=peers),
        [shape(3, count), shape(peers, 16, 2 * own), shape(192, elements, dtype=BF16)],
        scratch=[
            pltpu.VMEM((48, peers * own), F32),
            pltpu.VMEM((32, peers * own), F32),
            pltpu.VMEM((96, elements), F32),
        ],
        smem=1,
        operands=(me, *ctrl, contact_patch.reshape(1, count), contact_param, gp_pos, vel_coef),
        flops=10**9,
    )
    tail = groups * 8
    force, beside, across = call(
        force_kernel,
        [shape(groups, 4, GROUP), shape(tail + 16, GROUP), shape(tail + 32, GROUP)],
        operands=(to_groups(recv), table, part),
        flops=4 * 10**9,
    )
    from_across = swap(across, 2)
    back = lax.all_to_all(to_owners(force), "flow", split_axis=0, concat_axis=0, tiled=True)
    from_corner = swap(from_across, 1)
    from_beside = swap(beside, 1)
    rows = elements // peers
    total, patch_part = call(
        near_kernel,
        [shape(96, rows), shape(16, 2 * own)],
        scratch=[pltpu.VMEM((192, width), BF16)],
        smem=1,
        operands=(me, beside, from_across, part),
        flops=2 * 10**9,
    )
    flow_force, patch_force = call(
        last_kernel,
        [shape(81, rows), shape(27, own)],
        scratch=[pltpu.VMEM((192, width), BF16)],
        smem=1,
        operands=(me, from_beside, from_corner, total, patch_part),
        flops=2 * 10**9,
    )
    flow_force, pushes = lax.optimization_barrier((flow_force, pushes))
    shell_force = call(
        finish_kernel, shape(3, count),
        scratch=[pltpu.VMEM((owners * 4, slots), F32)],
        operands=(back, block, rank, pushes),
        flops=10**8,
    )
    return flow_force, shell_force, patch_force


def solution(mesh):
    both = ("flow", "leaf")
    in_specs = (
        P(None, "flow"), P(both, None), P(both), P(None, both), P(None, both), P(both),
        P(None, both), P(both), P(None, both), P(None, both),
    )
    out_specs = (P(None, both), P(None, both), P(None, both))

    return jax.shard_map(
        per_device, mesh=mesh, in_specs=in_specs, out_specs=out_specs, check_vma=False
    )
```

```python
import functools

import jax
import jax.numpy as jnp
from jax import lax
from jax.experimental import pallas as pl
from jax.experimental.pallas import tpu as pltpu
from jax.sharding import PartitionSpec as P


BETA = 1.5
STIFF = 2.0
REACH = 0.5
VMEM_LIMIT = 20 * 2**20
GROUP = 512

F32, BF16, F8 = jnp.float32, jnp.bfloat16, jnp.float8_e4m3fn
I32, I16 = jnp.int32, jnp.int16
NN = (((1,), (0,)), ((), ()))
NT = (((1,), (1,)), ((), ()))


def dot(a, b, dims):
    return lax.dot_general(a, b, dims, preferred_element_type=F32)


def split(x):
    high = x.astype(BF16)
    low = (x - high.astype(F32)).astype(BF16)
    return jnp.concatenate([high, low], axis=0)


def rows_of(shape):
    return lax.broadcasted_iota(I32, shape, 0)


def one_hot(index, rows, offset=0):
    number = lax.broadcasted_iota(I16, (rows, index.shape[1]), 0)
    hit = number == (index - offset).astype(I16)
    return jnp.where(hit, jnp.asarray(1, BF16), jnp.asarray(0, BF16)).astype(F8)


def pick_basis(x, which):
    b0 = 0.5 * (1.0 - x) ** 2
    b1 = 0.5 * (1.0 + 2.0 * x - 2.0 * x * x)
    b2 = 0.5 * x * x
    return jnp.where(which == 0, b0, jnp.where(which == 1, b1, b2))


def split_solid(x):
    high = x[:80].astype(BF16)
    low = (x[:80] - high.astype(F32)).astype(BF16)
    top = x[80:].astype(BF16).astype(F32)
    last = jnp.concatenate([top, x[80:] - top], axis=0).astype(BF16)
    return high, low, last


def join_solid(y):
    return jnp.concatenate([y[:80] + y[80:160], y[160:168] + y[168:176]], axis=0)


def solid_weights(x0, x1, x2):
    j = rows_of((8, 1))
    plane = pick_basis(x1, j // 3) * pick_basis(x2, j % 3)
    corner = (0.5 * x1 * x1) * (0.5 * x2 * x2)
    b0 = 0.5 * (1.0 - x0) ** 2
    b1 = 0.5 * (1.0 + 2.0 * x0 - 2.0 * x0 * x0)
    b2 = 0.5 * x0 * x0
    tiles = [plane * b0, plane * b1, plane * b2]
    return tiles, pick_basis(x0, j % 3) * corner, b2 * corner


def shell_weights(x0, x1):
    k = rows_of((16, 1))
    return pick_basis(x0, k // 3) * pick_basis(x1, k % 3)


def pack_kernel(block_ref, elem_ref, param_ref, vel_ref, weight_ref, out_ref, rank_ref, vals):
    owners, _, slots = out_ref.shape
    count = block_ref.shape[1]
    step = 256
    block = block_ref[...]
    mask = jnp.where(rows_of((owners, count)) == block, 1.0, 0.0)
    upto = (
        lax.broadcasted_iota(I32, (step, step), 0) <= lax.broadcasted_iota(I32, (step, step), 1)
    )
    upto = jnp.where(upto, 1.0, 0.0).astype(BF16)
    base = jnp.zeros((owners, 1), F32)
    ranks = []
    for i in range(count // step):
        part = mask[:, i * step : (i + 1) * step]
        running = dot(part.astype(BF16), upto, NN)
        ranks.append(jnp.sum(part * (running + (base - 1.0)), axis=0, keepdims=True))
        base = base + running[:, step - 1 : step]
    rank = jnp.concatenate(ranks, axis=1).astype(I32)
    rank_ref[...] = rank
    vals[0:1] = elem_ref[...].astype(F32) + 1.0
    vals[1:4] = param_ref[...]
    vals[4:7] = vel_ref[...]
    vals[7:8] = weight_ref[...]
    v = vals[...]
    terms = jnp.concatenate([v * mask[d : d + 1] for d in range(owners)], axis=0)
    packed = dot(split(terms), one_hot(rank, slots), NT)
    packed = packed[: owners * 8] + packed[owners * 8 :]
    for d in range(owners):
        out_ref[d] = packed[d * 8 : (d + 1) * 8]


def contact_kernel(me_ref, *refs, peers):
    ctrl_refs = refs[:peers]
    patch_ref, param_ref, pos_ref, coef_ref = refs[peers : peers + 4]
    push_ref, part_ref, table_ref, ctrl, tight, wide = refs[peers + 4 :]
    own = ctrl_refs[0].shape[1]
    me = me_ref[0]
    ctrl[...] = jnp.zeros_like(ctrl)
    for k in range(peers):
        for c in range(3):
            ctrl[c * 16 : c * 16 + 9, k * own : (k + 1) * own] = ctrl_refs[k][c * 9 : c * 9 + 9, :]
    patch = patch_ref[...]
    table = jnp.concatenate([one_hot(patch, own, (me ^ k) * own) for k in range(peers)], axis=0)
    picked = dot(split(ctrl[...]), table, NN)
    picked = picked[:48] + picked[48:]
    w = shell_weights(param_ref[0:1, :], param_ref[1:2, :])
    gaps = [
        pos_ref[c : c + 1, :] - jnp.sum(picked[c * 16 : c * 16 + 16] * w, axis=0, keepdims=True)
        for c in range(3)
    ]
    far = 1.0 + (gaps[0] * gaps[0] + gaps[1] * gaps[1] + gaps[2] * gaps[2]) / (REACH * REACH)
    pushes = [STIFF * g / far for g in gaps]
    for c in range(3):
        push_ref[c : c + 1, :] = pushes[c]
    terms = jnp.concatenate([-(w * f) for f in pushes], axis=0)
    part = dot(split(terms), table, NT)
    part = part[:48] + part[48:]
    for c in range(3):
        tight[c * 9 : c * 9 + 9] = part[c * 16 : c * 16 + 9]
    part_ref[...] = jnp.zeros_like(part_ref)
    for k in range(peers):
        part_ref[k, 0:14, 0:own] = tight[0:14, k * own : (k + 1) * own]
        part_ref[k, 0:13, own:] = tight[14:27, k * own : (k + 1) * own]
    wide[80:88] = jnp.zeros((8, wide.shape[1]), F32)
    for c in range(3):
        for a in range(3):
            k = c * 27 + a * 9
            wide[c * 24 + a * 8 : c * 24 + a * 8 + 8, :] = coef_ref[k : k + 8, :]
            wide[72 + c * 3 + a : 73 + c * 3 + a, :] = coef_ref[k + 8 : k + 9, :]
    table_ref[0:80], table_ref[80:160], table_ref[160:176] = split_solid(wide[...])


def force_kernel(recv_ref, table_ref, part_ref, back_ref, beside_ref, across_ref):
    groups = recv_ref.shape[0]
    elements = table_ref.shape[1]
    for g in range(groups):
        point = recv_ref[g]
        index = point[0:1].astype(I32) - 1
        picked = dot(table_ref[...], one_hot(index, elements), NN)
        picked = join_solid(picked)
        tiles, rest, final = solid_weights(point[1:2], point[2:3], point[3:4])
        rest = picked[72:80] * rest
        speed = []
        for c in range(3):
            part = jnp.where(rows_of((8, 1)) // 3 == c, rest, 0.0)
            for a in range(3):
                part = part + picked[c * 24 + a * 8 : c * 24 + a * 8 + 8] * tiles[a]
            speed.append(jnp.sum(part, axis=0, keepdims=True))
        speed[2] = speed[2] + picked[80:81] * final
        scale = BETA * point[7:8]
        beside_ref[g * 8 : g * 8 + 4] = point[0:4]
        for c in range(3):
            force = scale * (point[4 + c : 5 + c] - speed[c])
            beside_ref[g * 8 + 4 + c : g * 8 + 5 + c] = force
            back_ref[g, c : c + 1] = force
        beside_ref[g * 8 + 7 : g * 8 + 8] = jnp.zeros((1, GROUP), F32)
        back_ref[g, 3:4] = jnp.zeros((1, GROUP), F32)
        across_ref[g * 8 : (g + 1) * 8] = beside_ref[g * 8 : (g + 1) * 8]
    tail = groups * 8
    beside_ref[tail:] = part_ref[1]
    across_ref[tail : tail + 16] = part_ref[2]
    across_ref[tail + 16 :] = part_ref[3]


def spread(source_ref, terms, first, rows):
    groups = terms.shape[1] // GROUP
    index = []
    for g in range(groups):
        point = source_ref[g * 8 : (g + 1) * 8]
        index.append(point[0:1].astype(I32))
        tiles, rest, final = solid_weights(point[1:2], point[2:3], point[3:4])
        f = [point[4 + c : 5 + c] for c in range(3)]
        which = rows_of((8, 1)) // 3
        parts = [tile * f[c] for c in range(3) for tile in tiles]
        parts.append(rest * jnp.where(which == 0, f[0], jnp.where(which == 1, f[1], f[2])))
        parts.append(jnp.broadcast_to(final * f[2], (8, GROUP)))
        here = pl.ds(g * GROUP, GROUP)
        terms[0:80, here], terms[80:160, here], terms[160:176, here] = split_solid(
            jnp.concatenate(parts, axis=0)
        )
    return dot(terms[...], one_hot(jnp.concatenate(index, axis=1), rows, first), NT)


def near_kernel(me_ref, own_ref, across_ref, part_ref, total_ref, patch_ref, terms):
    rows = total_ref.shape[1]
    tail = terms.shape[1] // GROUP * 8
    first = me_ref[0] * rows + 1
    total = spread(own_ref, terms, first, rows)
    total = total + spread(across_ref, terms, first, rows)
    total_ref[...] = join_solid(total)
    patch_ref[...] = part_ref[0] + across_ref[tail : tail + 16]


def last_kernel(me_ref, beside_ref, corner_ref, total_ref, part_ref, flow_ref, patch_ref, terms):
    rows = total_ref.shape[1]
    own = patch_ref.shape[1]
    tail = terms.shape[1] // GROUP * 8
    first = me_ref[0] * rows + 1
    total = spread(beside_ref, terms, first, rows)
    total = total + spread(corner_ref, terms, first, rows)
    total = total_ref[...] + join_solid(total)
    for c in range(3):
        for a in range(3):
            k = c * 27 + a * 9
            flow_ref[k : k + 8, :] = total[c * 24 + a * 8 : c * 24 + a * 8 + 8]
            flow_ref[k + 8 : k + 9, :] = total[72 + c * 3 + a : 73 + c * 3 + a]
    part = part_ref[...] + beside_ref[tail:] + corner_ref[tail + 16 :]
    patch_ref[0:14] = part[0:14, 0:own]
    patch_ref[14:27] = part[0:13, own:]


def finish_kernel(back_ref, block_ref, rank_ref, push_ref, out_ref, rows):
    owners, _, slots = back_ref.shape
    for d in range(owners):
        rows[d * 4 : (d + 1) * 4] = back_ref[d]
    got = dot(split(rows[...]), one_hot(rank_ref[...], slots), NN)
    got = got[: owners * 4] + got[owners * 4 :]
    block = block_ref[...]
    half = rows_of((8, 1)) // 4
    total = jnp.zeros((8, block.shape[1]), F32)
    for d in range(owners // 2):
        total = total + jnp.where(block - half == 2 * d, got[d * 8 : (d + 1) * 8], 0.0)
    out_ref[...] = push_ref[...] - (total[0:3] + total[4:7])


def call(kernel, out_shape, scratch=(), smem=0, operands=(), flops=0, limit=VMEM_LIMIT):
    specs = [
        pl.BlockSpec(memory_space=pltpu.SMEM if i < smem else pltpu.VMEM)
        for i in range(len(operands))
    ]
    return pl.pallas_call(
        kernel,
        out_shape=out_shape,
        in_specs=specs,
        out_specs=jax.tree.map(lambda _: pl.BlockSpec(memory_space=pltpu.VMEM), out_shape),
        scratch_shapes=scratch,
        cost_estimate=pl.CostEstimate(flops=flops, bytes_accessed=0, transcendentals=0),
        compiler_params=pltpu.CompilerParams(vmem_limit_bytes=limit),
    )(*operands)


def shape(*dims, dtype=F32):
    return jax.ShapeDtypeStruct(dims, dtype)


def per_device(
    vel_coef, gp_block, gp_elem, gp_param, gp_vel, gp_weight, gp_pos, contact_patch,
    contact_param, patch_ctrl,
):
    owners = lax.axis_size("flow")
    peers = lax.axis_size("leaf")
    count = gp_elem.shape[0]
    slots = 2 * count // owners
    width = slots * owners
    groups = width // GROUP
    elements = vel_coef.shape[1]
    own = patch_ctrl.shape[1]
    me = lax.axis_index("leaf").astype(I32).reshape(1)

    def swap(x, k):
        return lax.ppermute(x, "leaf", [(i, i ^ k) for i in range(peers)])

    def to_groups(x):
        if slots == GROUP:
            return x
        return x.transpose(1, 0, 2).reshape(-1, groups, GROUP).transpose(1, 0, 2)

    def to_owners(x):
        if slots == GROUP:
            return x
        return x.transpose(1, 0, 2).reshape(-1, owners, slots).transpose(1, 0, 2)

    block = gp_block.reshape(1, count)
    payload, rank = call(
        pack_kernel,
        [shape(owners, 8, slots), shape(1, count, dtype=I32)],
        scratch=[pltpu.VMEM((8, count), F32)],
        operands=(block, gp_elem.reshape(1, count), gp_param, gp_vel, gp_weight.reshape(1, count)),
        flops=10**9,
        limit=None,
    )
    payload, here = lax.optimization_barrier((payload, patch_ctrl))
    far = swap(here, 2)
    recv = lax.all_to_all(payload, "flow", split_axis=0, concat_axis=0, tiled=True)
    twin = swap(here, 1)
    diag = swap(far, 1)
    ctrl = (here, twin, far, diag)
    pushes, part, table = call(
        functools.partial(contact_kernel, peers=peers),
        [shape(3, count), shape(peers, 16, 2 * own), shape(176, elements, dtype=BF16)],
        scratch=[
            pltpu.VMEM((48, peers * own), F32),
            pltpu.VMEM((32, peers * own), F32),
            pltpu.VMEM((88, elements), F32),
        ],
        smem=1,
        operands=(me, *ctrl, contact_patch.reshape(1, count), contact_param, gp_pos, vel_coef),
        flops=10**9,
    )
    tail = groups * 8
    force, beside, across = call(
        force_kernel,
        [shape(groups, 4, GROUP), shape(tail + 16, GROUP), shape(tail + 32, GROUP)],
        operands=(to_groups(recv), table, part),
        flops=4 * 10**9,
    )
    from_across = swap(across, 2)
    back = lax.all_to_all(to_owners(force), "flow", split_axis=0, concat_axis=0, tiled=True)
    from_corner = swap(from_across, 1)
    from_beside = swap(beside, 1)
    rows = elements // peers
    total, patch_part = call(
        near_kernel,
        [shape(88, rows), shape(16, 2 * own)],
        scratch=[pltpu.VMEM((176, width), BF16)],
        smem=1,
        operands=(me, beside, from_across, part),
        flops=2 * 10**9,
    )
    flow_force, patch_force = call(
        last_kernel,
        [shape(81, rows), shape(27, own)],
        scratch=[pltpu.VMEM((176, width), BF16)],
        smem=1,
        operands=(me, from_beside, from_corner, total, patch_part),
        flops=2 * 10**9,
    )
    flow_force, pushes = lax.optimization_barrier((flow_force, pushes))
    shell_force = call(
        finish_kernel, shape(3, count),
        scratch=[pltpu.VMEM((owners * 4, slots), F32)],
        operands=(back, block, rank, pushes),
        flops=10**8,
    )
    return flow_force, shell_force, patch_force


def solution(mesh):
    both = ("flow", "leaf")
    in_specs = (
        P(None, "flow"), P(both, None), P(both), P(None, both), P(None, both), P(both),
        P(None, both), P(both), P(None, both), P(None, both),
    )
    out_specs = (P(None, both), P(None, both), P(None, both))

    return jax.shard_map(
        per_device, mesh=mesh, in_specs=in_specs, out_specs=out_specs, check_vma=False
    )
```

```python
import functools

import jax
import jax.numpy as jnp
from jax import lax
from jax.experimental import pallas as pl
from jax.experimental.pallas import tpu as pltpu
from jax.sharding import PartitionSpec as P


BETA = 1.5
STIFF = 2.0
REACH = 0.5
VMEM_LIMIT = 20 * 2**20
GROUP = 512

F32, BF16, F8 = jnp.float32, jnp.bfloat16, jnp.float8_e4m3fn
I32, I16 = jnp.int32, jnp.int16
NN = (((1,), (0,)), ((), ()))
NT = (((1,), (1,)), ((), ()))


def dot(a, b, dims):
    return lax.dot_general(a, b, dims, preferred_element_type=F32)


def split(x):
    high = x.astype(BF16)
    low = (x - high.astype(F32)).astype(BF16)
    return jnp.concatenate([high, low], axis=0)


def rows_of(shape):
    return lax.broadcasted_iota(I32, shape, 0)


def one_hot(index, rows, offset=0):
    number = lax.broadcasted_iota(I16, (rows, index.shape[1]), 0)
    hit = number == (index - offset).astype(I16)
    return jnp.where(hit, jnp.asarray(1, BF16), jnp.asarray(0, BF16)).astype(F8)


def pick_basis(x, which):
    b0 = 0.5 * (1.0 - x) ** 2
    b1 = 0.5 * (1.0 + 2.0 * x - 2.0 * x * x)
    b2 = 0.5 * x * x
    return jnp.where(which == 0, b0, jnp.where(which == 1, b1, b2))


def split_solid(x):
    high = x[:80].astype(BF16)
    low = (x[:80] - high.astype(F32)).astype(BF16)
    top = x[80:].astype(BF16).astype(F32)
    last = jnp.concatenate([top, x[80:] - top], axis=0).astype(BF16)
    return high, low, last


def join_solid(y):
    return jnp.concatenate([y[:80] + y[80:160], y[160:168] + y[168:176]], axis=0)


def solid_weights(x0, x1, x2):
    j = rows_of((8, 1))
    plane = pick_basis(x1, j // 3) * pick_basis(x2, j % 3)
    corner = (0.5 * x1 * x1) * (0.5 * x2 * x2)
    b0 = 0.5 * (1.0 - x0) ** 2
    b1 = 0.5 * (1.0 + 2.0 * x0 - 2.0 * x0 * x0)
    b2 = 0.5 * x0 * x0
    tiles = [plane * b0, plane * b1, plane * b2]
    return tiles, pick_basis(x0, j % 3) * corner, b2 * corner


def shell_weights(x0, x1):
    k = rows_of((16, 1))
    return pick_basis(x0, k // 3) * pick_basis(x1, k % 3)


def pack_kernel(block_ref, elem_ref, param_ref, vel_ref, weight_ref, out_ref, rank_ref, vals):
    owners, _, slots = out_ref.shape
    count = block_ref.shape[1]
    step = 256
    block = block_ref[...]
    mask = jnp.where(rows_of((owners, count)) == block, 1.0, 0.0)
    upto = (
        lax.broadcasted_iota(I32, (step, step), 0) <= lax.broadcasted_iota(I32, (step, step), 1)
    )
    upto = jnp.where(upto, 1.0, 0.0).astype(BF16)
    base = jnp.zeros((owners, 1), F32)
    ranks = []
    for i in range(count // step):
        part = mask[:, i * step : (i + 1) * step]
        running = dot(part.astype(BF16), upto, NN)
        ranks.append(jnp.sum(part * (running + (base - 1.0)), axis=0, keepdims=True))
        base = base + running[:, step - 1 : step]
    rank = jnp.concatenate(ranks, axis=1).astype(I32)
    rank_ref[...] = rank
    vals[0:1] = elem_ref[...].astype(F32) + 1.0
    vals[1:4] = param_ref[...]
    vals[4:7] = vel_ref[...]
    vals[7:8] = weight_ref[...]
    v = vals[...]
    terms = jnp.concatenate([v * mask[d : d + 1] for d in range(owners)], axis=0)
    packed = dot(split(terms), one_hot(rank, slots), NT)
    packed = packed[: owners * 8] + packed[owners * 8 :]
    for d in range(owners):
        out_ref[d] = packed[d * 8 : (d + 1) * 8]


def contact_kernel(me_ref, *refs, peers):
    ctrl_refs = refs[:peers]
    patch_ref, param_ref, pos_ref, coef_ref = refs[peers : peers + 4]
    push_ref, part_ref, table_ref, ctrl, tight, wide = refs[peers + 4 :]
    own = ctrl_refs[0].shape[1]
    me = me_ref[0]
    ctrl[...] = jnp.zeros_like(ctrl)
    for k in range(peers):
        for c in range(3):
            ctrl[c * 16 : c * 16 + 9, k * own : (k + 1) * own] = ctrl_refs[k][c * 9 : c * 9 + 9, :]
    patch = patch_ref[...]
    table = jnp.concatenate([one_hot(patch, own, (me ^ k) * own) for k in range(peers)], axis=0)
    picked = dot(split(ctrl[...]), table, NN)
    picked = picked[:48] + picked[48:]
    w = shell_weights(param_ref[0:1, :], param_ref[1:2, :])
    gaps = [
        pos_ref[c : c + 1, :] - jnp.sum(picked[c * 16 : c * 16 + 16] * w, axis=0, keepdims=True)
        for c in range(3)
    ]
    far = 1.0 + (gaps[0] * gaps[0] + gaps[1] * gaps[1] + gaps[2] * gaps[2]) / (REACH * REACH)
    pushes = [STIFF * g / far for g in gaps]
    for c in range(3):
        push_ref[c : c + 1, :] = pushes[c]
    terms = jnp.concatenate([-(w * f) for f in pushes], axis=0)
    part = dot(split(terms), table, NT)
    part = part[:48] + part[48:]
    for c in range(3):
        tight[c * 9 : c * 9 + 9] = part[c * 16 : c * 16 + 9]
    part_ref[...] = jnp.zeros_like(part_ref)
    for k in range(peers):
        part_ref[k, 0:14, 0:own] = tight[0:14, k * own : (k + 1) * own]
        part_ref[k, 0:13, own:] = tight[14:27, k * own : (k + 1) * own]
    wide[80:88] = jnp.zeros((8, wide.shape[1]), F32)
    for c in range(3):
        for a in range(3):
            k = c * 27 + a * 9
            wide[c * 24 + a * 8 : c * 24 + a * 8 + 8, :] = coef_ref[k : k + 8, :]
            wide[72 + c * 3 + a : 73 + c * 3 + a, :] = coef_ref[k + 8 : k + 9, :]
    table_ref[0:80], table_ref[80:160], table_ref[160:176] = split_solid(wide[...])


def force_of(point, table_ref):
    index = point[0:1].astype(I32) - 1
    picked = join_solid(dot(table_ref[...], one_hot(index, table_ref.shape[1]), NN))
    tiles, rest, final = solid_weights(point[1:2], point[2:3], point[3:4])
    rest = picked[72:80] * rest
    forces = []
    for c in range(3):
        part = jnp.where(rows_of((8, 1)) // 3 == c, rest, 0.0)
        for a in range(3):
            part = part + picked[c * 24 + a * 8 : c * 24 + a * 8 + 8] * tiles[a]
        speed = jnp.sum(part, axis=0, keepdims=True)
        if c == 2:
            speed = speed + picked[80:81] * final
        forces.append(BETA * point[7:8] * (point[4 + c : 5 + c] - speed))
    return forces


def home_kernel(row_ref, sent_ref, table_ref, out_ref):
    for c, force in enumerate(force_of(sent_ref[row_ref[0]], table_ref)):
        out_ref[c : c + 1] = force
    out_ref[3:8] = jnp.zeros((5, GROUP), F32)


def force_kernel(row_ref, recv_ref, table_ref, part_ref, *refs):
    *homes, back_ref, beside_ref, across_ref = refs
    groups = recv_ref.shape[0]

    def put(g, point, forces):
        both = jnp.concatenate([point[0:4], *forces, jnp.zeros((1, GROUP), F32)], axis=0)
        here = pl.ds(pl.multiple_of(g * 8, 8), 8)
        beside_ref[here] = both
        across_ref[here] = both
        back_ref[g] = both[4:8]

    first = row_ref[0]
    for r in range(groups):
        g = lax.rem(first + r, groups)
        point = recv_ref[g]
        if homes and r == 0:
            put(g, point, [homes[0][c : c + 1] for c in range(3)])
        else:
            put(g, point, force_of(point, table_ref))
    tail = groups * 8
    beside_ref[tail:] = part_ref[1]
    across_ref[tail : tail + 16] = part_ref[2]
    across_ref[tail + 16 :] = part_ref[3]


def spread(source_ref, terms, first, rows):
    groups = terms.shape[1] // GROUP
    index = []
    for g in range(groups):
        point = source_ref[g * 8 : (g + 1) * 8]
        index.append(point[0:1].astype(I32))
        tiles, rest, final = solid_weights(point[1:2], point[2:3], point[3:4])
        f = [point[4 + c : 5 + c] for c in range(3)]
        which = rows_of((8, 1)) // 3
        parts = [tile * f[c] for c in range(3) for tile in tiles]
        parts.append(rest * jnp.where(which == 0, f[0], jnp.where(which == 1, f[1], f[2])))
        parts.append(jnp.broadcast_to(final * f[2], (8, GROUP)))
        here = pl.ds(g * GROUP, GROUP)
        terms[0:80, here], terms[80:160, here], terms[160:176, here] = split_solid(
            jnp.concatenate(parts, axis=0)
        )
    return dot(terms[...], one_hot(jnp.concatenate(index, axis=1), rows, first), NT)


def near_kernel(me_ref, own_ref, across_ref, part_ref, total_ref, patch_ref, terms):
    rows = total_ref.shape[1]
    tail = terms.shape[1] // GROUP * 8
    first = me_ref[0] * rows + 1
    total = spread(own_ref, terms, first, rows)
    total = total + spread(across_ref, terms, first, rows)
    total_ref[...] = join_solid(total)
    patch_ref[...] = part_ref[0] + across_ref[tail : tail + 16]


def last_kernel(me_ref, beside_ref, corner_ref, total_ref, part_ref, flow_ref, patch_ref, terms):
    rows = total_ref.shape[1]
    own = patch_ref.shape[1]
    tail = terms.shape[1] // GROUP * 8
    first = me_ref[0] * rows + 1
    total = spread(beside_ref, terms, first, rows)
    total = total + spread(corner_ref, terms, first, rows)
    total = total_ref[...] + join_solid(total)
    for c in range(3):
        for a in range(3):
            k = c * 27 + a * 9
            flow_ref[k : k + 8, :] = total[c * 24 + a * 8 : c * 24 + a * 8 + 8]
            flow_ref[k + 8 : k + 9, :] = total[72 + c * 3 + a : 73 + c * 3 + a]
    part = part_ref[...] + beside_ref[tail:] + corner_ref[tail + 16 :]
    patch_ref[0:14] = part[0:14, 0:own]
    patch_ref[14:27] = part[0:13, own:]


def finish_kernel(back_ref, block_ref, rank_ref, push_ref, out_ref, rows):
    owners, _, slots = back_ref.shape
    for d in range(owners):
        rows[d * 4 : (d + 1) * 4] = back_ref[d]
    got = dot(split(rows[...]), one_hot(rank_ref[...], slots), NN)
    got = got[: owners * 4] + got[owners * 4 :]
    block = block_ref[...]
    half = rows_of((8, 1)) // 4
    total = jnp.zeros((8, block.shape[1]), F32)
    for d in range(owners // 2):
        total = total + jnp.where(block - half == 2 * d, got[d * 8 : (d + 1) * 8], 0.0)
    out_ref[...] = push_ref[...] - (total[0:3] + total[4:7])


def call(kernel, out_shape, scratch=(), smem=0, operands=(), flops=0, limit=VMEM_LIMIT):
    specs = [
        pl.BlockSpec(memory_space=pltpu.SMEM if i < smem else pltpu.VMEM)
        for i in range(len(operands))
    ]
    return pl.pallas_call(
        kernel,
        out_shape=out_shape,
        in_specs=specs,
        out_specs=jax.tree.map(lambda _: pl.BlockSpec(memory_space=pltpu.VMEM), out_shape),
        scratch_shapes=scratch,
        cost_estimate=pl.CostEstimate(flops=flops, bytes_accessed=0, transcendentals=0),
        compiler_params=pltpu.CompilerParams(vmem_limit_bytes=limit),
    )(*operands)


def shape(*dims, dtype=F32):
    return jax.ShapeDtypeStruct(dims, dtype)


def per_device(
    vel_coef, gp_block, gp_elem, gp_param, gp_vel, gp_weight, gp_pos, contact_patch,
    contact_param, patch_ctrl,
):
    owners = lax.axis_size("flow")
    peers = lax.axis_size("leaf")
    count = gp_elem.shape[0]
    slots = 2 * count // owners
    width = slots * owners
    groups = width // GROUP
    elements = vel_coef.shape[1]
    own = patch_ctrl.shape[1]
    me = lax.axis_index("leaf").astype(I32).reshape(1)

    def swap(x, k):
        return lax.ppermute(x, "leaf", [(i, i ^ k) for i in range(peers)])

    def to_groups(x):
        if slots == GROUP:
            return x
        return x.transpose(1, 0, 2).reshape(-1, groups, GROUP).transpose(1, 0, 2)

    def to_owners(x):
        if slots == GROUP:
            return x
        return x.transpose(1, 0, 2).reshape(-1, owners, slots).transpose(1, 0, 2)

    block = gp_block.reshape(1, count)
    payload, rank = call(
        pack_kernel,
        [shape(owners, 8, slots), shape(1, count, dtype=I32)],
        scratch=[pltpu.VMEM((8, count), F32)],
        operands=(block, gp_elem.reshape(1, count), gp_param, gp_vel, gp_weight.reshape(1, count)),
        flops=10**9,
        limit=None,
    )
    payload, here = lax.optimization_barrier((payload, patch_ctrl))
    far = swap(here, 2)
    recv = lax.all_to_all(payload, "flow", split_axis=0, concat_axis=0, tiled=True)
    twin = swap(here, 1)
    diag = swap(far, 1)
    ctrl = (here, twin, far, diag)
    pushes, part, table = call(
        functools.partial(contact_kernel, peers=peers),
        [shape(3, count), shape(peers, 16, 2 * own), shape(176, elements, dtype=BF16)],
        scratch=[
            pltpu.VMEM((48, peers * own), F32),
            pltpu.VMEM((32, peers * own), F32),
            pltpu.VMEM((88, elements), F32),
        ],
        smem=1,
        operands=(me, *ctrl, contact_patch.reshape(1, count), contact_param, gp_pos, vel_coef),
        flops=10**9,
    )
    tail = groups * 8
    row = lax.axis_index("flow").astype(I32).reshape(1) % groups
    homes = ()
    if slots == GROUP:
        homes = (
            call(
                home_kernel, shape(8, GROUP), smem=1,
                operands=(row, payload, table), flops=10**9,
            ),
        )
    force, beside, across = call(
        force_kernel,
        [shape(groups, 4, GROUP), shape(tail + 16, GROUP), shape(tail + 32, GROUP)],
        smem=1,
        operands=(row, to_groups(recv), table, part, *homes),
        flops=4 * 10**9,
    )
    from_across = swap(across, 2)
    back = lax.all_to_all(to_owners(force), "flow", split_axis=0, concat_axis=0, tiled=True)
    from_corner = swap(from_across, 1)
    from_beside = swap(beside, 1)
    rows = elements // peers
    total, patch_part = call(
        near_kernel,
        [shape(88, rows), shape(16, 2 * own)],
        scratch=[pltpu.VMEM((176, width), BF16)],
        smem=1,
        operands=(me, beside, from_across, part),
        flops=2 * 10**9,
    )
    flow_force, patch_force = call(
        last_kernel,
        [shape(81, rows), shape(27, own)],
        scratch=[pltpu.VMEM((176, width), BF16)],
        smem=1,
        operands=(me, from_beside, from_corner, total, patch_part),
        flops=2 * 10**9,
    )
    flow_force, pushes = lax.optimization_barrier((flow_force, pushes))
    shell_force = call(
        finish_kernel, shape(3, count),
        scratch=[pltpu.VMEM((owners * 4, slots), F32)],
        operands=(back, block, rank, pushes),
        flops=10**8,
    )
    return flow_force, shell_force, patch_force


def solution(mesh):
    both = ("flow", "leaf")
    in_specs = (
        P(None, "flow"), P(both, None), P(both), P(None, both), P(None, both), P(both),
        P(None, both), P(both), P(None, both), P(None, both),
    )
    out_specs = (P(None, both), P(None, both), P(None, both))

    return jax.shard_map(
        per_device, mesh=mesh, in_specs=in_specs, out_specs=out_specs, check_vma=False
    )
```

```python
import functools

import jax
import jax.numpy as jnp
from jax import lax
from jax.experimental import pallas as pl
from jax.experimental.pallas import tpu as pltpu
from jax.sharding import PartitionSpec as P


BETA = 1.5
STIFF = 2.0
REACH = 0.5
VMEM_LIMIT = 20 * 2**20
GROUP = 512

F32, BF16, F8 = jnp.float32, jnp.bfloat16, jnp.float8_e4m3fn
I32, I16 = jnp.int32, jnp.int16
NN = (((1,), (0,)), ((), ()))
NT = (((1,), (1,)), ((), ()))


def dot(a, b, dims):
    return lax.dot_general(a, b, dims, preferred_element_type=F32)


def split(x):
    high = x.astype(BF16)
    low = (x - high.astype(F32)).astype(BF16)
    return jnp.concatenate([high, low], axis=0)


def rows_of(shape):
    return lax.broadcasted_iota(I32, shape, 0)


def one_hot(index, rows, offset=0):
    number = lax.broadcasted_iota(I16, (rows, index.shape[1]), 0)
    hit = number == (index - offset).astype(I16)
    return jnp.where(hit, jnp.asarray(1, BF16), jnp.asarray(0, BF16)).astype(F8)


def pick_basis(x, which):
    b0 = 0.5 * (1.0 - x) ** 2
    b1 = 0.5 * (1.0 + 2.0 * x - 2.0 * x * x)
    b2 = 0.5 * x * x
    return jnp.where(which == 0, b0, jnp.where(which == 1, b1, b2))


def split_solid(x):
    high = x[:80].astype(BF16)
    low = (x[:80] - high.astype(F32)).astype(BF16)
    top = x[80:].astype(BF16).astype(F32)
    last = jnp.concatenate([top, x[80:] - top], axis=0).astype(BF16)
    return high, low, last


def join_solid(y):
    return jnp.concatenate([y[:80] + y[80:160], y[160:168] + y[168:176]], axis=0)


def solid_weights(x0, x1, x2):
    j = rows_of((8, 1))
    plane = pick_basis(x1, j // 3) * pick_basis(x2, j % 3)
    corner = (0.5 * x1 * x1) * (0.5 * x2 * x2)
    b0 = 0.5 * (1.0 - x0) ** 2
    b1 = 0.5 * (1.0 + 2.0 * x0 - 2.0 * x0 * x0)
    b2 = 0.5 * x0 * x0
    tiles = [plane * b0, plane * b1, plane * b2]
    return tiles, pick_basis(x0, j % 3) * corner, b2 * corner


def shell_weights(x0, x1):
    k = rows_of((16, 1))
    return pick_basis(x0, k // 3) * pick_basis(x1, k % 3)


def pack_kernel(block_ref, elem_ref, param_ref, vel_ref, weight_ref, out_ref, rank_ref, vals):
    owners, _, slots = out_ref.shape
    count = block_ref.shape[1]
    step = 256
    block = block_ref[...]
    mask = jnp.where(rows_of((owners, count)) == block, 1.0, 0.0)
    upto = (
        lax.broadcasted_iota(I32, (step, step), 0) <= lax.broadcasted_iota(I32, (step, step), 1)
    )
    upto = jnp.where(upto, 1.0, 0.0).astype(BF16)
    base = jnp.zeros((owners, 1), F32)
    ranks = []
    for i in range(count // step):
        part = mask[:, i * step : (i + 1) * step]
        running = dot(part.astype(BF16), upto, NN)
        ranks.append(jnp.sum(part * (running + (base - 1.0)), axis=0, keepdims=True))
        base = base + running[:, step - 1 : step]
    rank = jnp.concatenate(ranks, axis=1).astype(I32)
    rank_ref[...] = rank
    vals[0:1] = elem_ref[...].astype(F32) + 1.0
    vals[1:4] = param_ref[...]
    vals[4:7] = vel_ref[...]
    vals[7:8] = weight_ref[...]
    v = vals[...]
    terms = jnp.concatenate([v * mask[d : d + 1] for d in range(owners)], axis=0)
    packed = dot(split(terms), one_hot(rank, slots), NT)
    packed = packed[: owners * 8] + packed[owners * 8 :]
    for d in range(owners):
        out_ref[d] = packed[d * 8 : (d + 1) * 8]


def contact_kernel(me_ref, *refs, peers):
    ctrl_refs = refs[:peers]
    patch_ref, param_ref, pos_ref, coef_ref, rank_ref = refs[peers : peers + 5]
    push_ref, part_ref, table_ref, place_ref, ctrl, tight, wide = refs[peers + 5 :]
    place_ref[...] = one_hot(rank_ref[...], place_ref.shape[0])
    own = ctrl_refs[0].shape[1]
    me = me_ref[0]
    ctrl[...] = jnp.zeros_like(ctrl)
    for k in range(peers):
        for c in range(3):
            ctrl[c * 16 : c * 16 + 9, k * own : (k + 1) * own] = ctrl_refs[k][c * 9 : c * 9 + 9, :]
    patch = patch_ref[...]
    table = jnp.concatenate([one_hot(patch, own, (me ^ k) * own) for k in range(peers)], axis=0)
    picked = dot(split(ctrl[...]), table, NN)
    picked = picked[:48] + picked[48:]
    w = shell_weights(param_ref[0:1, :], param_ref[1:2, :])
    gaps = [
        pos_ref[c : c + 1, :] - jnp.sum(picked[c * 16 : c * 16 + 16] * w, axis=0, keepdims=True)
        for c in range(3)
    ]
    far = 1.0 + (gaps[0] * gaps[0] + gaps[1] * gaps[1] + gaps[2] * gaps[2]) / (REACH * REACH)
    pushes = [STIFF * g / far for g in gaps]
    for c in range(3):
        push_ref[c : c + 1, :] = pushes[c]
    terms = jnp.concatenate([-(w * f) for f in pushes], axis=0)
    part = dot(split(terms), table, NT)
    part = part[:48] + part[48:]
    for c in range(3):
        tight[c * 9 : c * 9 + 9] = part[c * 16 : c * 16 + 9]
    part_ref[...] = jnp.zeros_like(part_ref)
    for k in range(peers):
        part_ref[k, 0:14, 0:own] = tight[0:14, k * own : (k + 1) * own]
        part_ref[k, 0:13, own:] = tight[14:27, k * own : (k + 1) * own]
    wide[80:88] = jnp.zeros((8, wide.shape[1]), F32)
    for c in range(3):
        for a in range(3):
            k = c * 27 + a * 9
            wide[c * 24 + a * 8 : c * 24 + a * 8 + 8, :] = coef_ref[k : k + 8, :]
            wide[72 + c * 3 + a : 73 + c * 3 + a, :] = coef_ref[k + 8 : k + 9, :]
    table_ref[0:80], table_ref[80:160], table_ref[160:176] = split_solid(wide[...])


def force_of(point, table_ref):
    index = point[0:1].astype(I32) - 1
    picked = join_solid(dot(table_ref[...], one_hot(index, table_ref.shape[1]), NN))
    tiles, rest, final = solid_weights(point[1:2], point[2:3], point[3:4])
    rest = picked[72:80] * rest
    forces = []
    for c in range(3):
        part = jnp.where(rows_of((8, 1)) // 3 == c, rest, 0.0)
        for a in range(3):
            part = part + picked[c * 24 + a * 8 : c * 24 + a * 8 + 8] * tiles[a]
        speed = jnp.sum(part, axis=0, keepdims=True)
        if c == 2:
            speed = speed + picked[80:81] * final
        forces.append(BETA * point[7:8] * (point[4 + c : 5 + c] - speed))
    return forces


def home_kernel(row_ref, sent_ref, table_ref, out_ref):
    for c, force in enumerate(force_of(sent_ref[row_ref[0]], table_ref)):
        out_ref[c : c + 1] = force
    out_ref[3:8] = jnp.zeros((5, GROUP), F32)


def force_kernel(row_ref, recv_ref, table_ref, part_ref, *refs):
    *homes, back_ref, beside_ref, across_ref = refs
    groups = recv_ref.shape[0]

    def put(g, point, forces):
        both = jnp.concatenate([point[0:4], *forces, jnp.zeros((1, GROUP), F32)], axis=0)
        here = pl.ds(pl.multiple_of(g * 8, 8), 8)
        beside_ref[here] = both
        across_ref[here] = both
        back_ref[g] = both[4:8]

    first = row_ref[0]
    for r in range(groups):
        g = lax.rem(first + r, groups)
        point = recv_ref[g]
        if homes and r == 0:
            put(g, point, [homes[0][c : c + 1] for c in range(3)])
        else:
            put(g, point, force_of(point, table_ref))
    tail = groups * 8
    beside_ref[tail:] = part_ref[1]
    across_ref[tail : tail + 16] = part_ref[2]
    across_ref[tail + 16 :] = part_ref[3]


def spread(source_ref, terms, first, rows):
    groups = terms.shape[1] // GROUP
    index = []
    for g in range(groups):
        point = source_ref[g * 8 : (g + 1) * 8]
        index.append(point[0:1].astype(I32))
        tiles, rest, final = solid_weights(point[1:2], point[2:3], point[3:4])
        f = [point[4 + c : 5 + c] for c in range(3)]
        which = rows_of((8, 1)) // 3
        parts = [tile * f[c] for c in range(3) for tile in tiles]
        parts.append(rest * jnp.where(which == 0, f[0], jnp.where(which == 1, f[1], f[2])))
        parts.append(jnp.broadcast_to(final * f[2], (8, GROUP)))
        here = pl.ds(g * GROUP, GROUP)
        terms[0:80, here], terms[80:160, here], terms[160:176, here] = split_solid(
            jnp.concatenate(parts, axis=0)
        )
    return dot(terms[...], one_hot(jnp.concatenate(index, axis=1), rows, first), NT)


def near_kernel(me_ref, own_ref, across_ref, part_ref, total_ref, patch_ref, terms):
    rows = total_ref.shape[1]
    tail = terms.shape[1] // GROUP * 8
    first = me_ref[0] * rows + 1
    total = spread(own_ref, terms, first, rows)
    total = total + spread(across_ref, terms, first, rows)
    total_ref[...] = join_solid(total)
    patch_ref[...] = part_ref[0] + across_ref[tail : tail + 16]


def last_kernel(me_ref, beside_ref, corner_ref, total_ref, part_ref, flow_ref, patch_ref, terms):
    rows = total_ref.shape[1]
    own = patch_ref.shape[1]
    tail = terms.shape[1] // GROUP * 8
    first = me_ref[0] * rows + 1
    total = spread(beside_ref, terms, first, rows)
    total = total + spread(corner_ref, terms, first, rows)
    total = total_ref[...] + join_solid(total)
    for c in range(3):
        for a in range(3):
            k = c * 27 + a * 9
            flow_ref[k : k + 8, :] = total[c * 24 + a * 8 : c * 24 + a * 8 + 8]
            flow_ref[k + 8 : k + 9, :] = total[72 + c * 3 + a : 73 + c * 3 + a]
    part = part_ref[...] + beside_ref[tail:] + corner_ref[tail + 16 :]
    patch_ref[0:14] = part[0:14, 0:own]
    patch_ref[14:27] = part[0:13, own:]


def finish_kernel(back_ref, block_ref, place_ref, push_ref, out_ref, rows):
    owners = back_ref.shape[0]
    for d in range(owners):
        rows[d * 4 : (d + 1) * 4] = back_ref[d]
    got = dot(split(rows[...]), place_ref[...], NN)
    got = got[: owners * 4] + got[owners * 4 :]
    block = block_ref[...]
    half = rows_of((8, 1)) // 4
    total = jnp.zeros((8, block.shape[1]), F32)
    for d in range(owners // 2):
        total = total + jnp.where(block - half == 2 * d, got[d * 8 : (d + 1) * 8], 0.0)
    out_ref[...] = push_ref[...] - (total[0:3] + total[4:7])


def call(kernel, out_shape, scratch=(), smem=0, operands=(), flops=0, limit=VMEM_LIMIT):
    specs = [
        pl.BlockSpec(memory_space=pltpu.SMEM if i < smem else pltpu.VMEM)
        for i in range(len(operands))
    ]
    return pl.pallas_call(
        kernel,
        out_shape=out_shape,
        in_specs=specs,
        out_specs=jax.tree.map(lambda _: pl.BlockSpec(memory_space=pltpu.VMEM), out_shape),
        scratch_shapes=scratch,
        cost_estimate=pl.CostEstimate(flops=flops, bytes_accessed=0, transcendentals=0),
        compiler_params=pltpu.CompilerParams(vmem_limit_bytes=limit),
    )(*operands)


def shape(*dims, dtype=F32):
    return jax.ShapeDtypeStruct(dims, dtype)


def per_device(
    vel_coef, gp_block, gp_elem, gp_param, gp_vel, gp_weight, gp_pos, contact_patch,
    contact_param, patch_ctrl,
):
    owners = lax.axis_size("flow")
    peers = lax.axis_size("leaf")
    count = gp_elem.shape[0]
    slots = 2 * count // owners
    width = slots * owners
    groups = width // GROUP
    elements = vel_coef.shape[1]
    own = patch_ctrl.shape[1]
    me = lax.axis_index("leaf").astype(I32).reshape(1)

    def swap(x, k):
        return lax.ppermute(x, "leaf", [(i, i ^ k) for i in range(peers)])

    def to_groups(x):
        if slots == GROUP:
            return x
        return x.transpose(1, 0, 2).reshape(-1, groups, GROUP).transpose(1, 0, 2)

    def to_owners(x):
        if slots == GROUP:
            return x
        return x.transpose(1, 0, 2).reshape(-1, owners, slots).transpose(1, 0, 2)

    block = gp_block.reshape(1, count)
    payload, rank = call(
        pack_kernel,
        [shape(owners, 8, slots), shape(1, count, dtype=I32)],
        scratch=[pltpu.VMEM((8, count), F32)],
        operands=(block, gp_elem.reshape(1, count), gp_param, gp_vel, gp_weight.reshape(1, count)),
        flops=10**9,
        limit=None,
    )
    payload, here = lax.optimization_barrier((payload, patch_ctrl))
    far = swap(here, 2)
    recv = lax.all_to_all(payload, "flow", split_axis=0, concat_axis=0, tiled=True)
    twin = swap(here, 1)
    diag = swap(far, 1)
    ctrl = (here, twin, far, diag)
    pushes, part, table, place = call(
        functools.partial(contact_kernel, peers=peers),
        [
            shape(3, count), shape(peers, 16, 2 * own), shape(176, elements, dtype=BF16),
            shape(slots, count, dtype=F8),
        ],
        scratch=[
            pltpu.VMEM((48, peers * own), F32),
            pltpu.VMEM((32, peers * own), F32),
            pltpu.VMEM((88, elements), F32),
        ],
        smem=1,
        operands=(me, *ctrl, contact_patch.reshape(1, count), contact_param, gp_pos, vel_coef, rank),
        flops=10**9,
    )
    tail = groups * 8
    row = lax.axis_index("flow").astype(I32).reshape(1) % groups
    homes = ()
    if slots == GROUP:
        homes = (
            call(
                home_kernel, shape(8, GROUP), smem=1,
                operands=(row, payload, table), flops=10**9,
            ),
        )
    force, beside, across = call(
        force_kernel,
        [shape(groups, 4, GROUP), shape(tail + 16, GROUP), shape(tail + 32, GROUP)],
        smem=1,
        operands=(row, to_groups(recv), table, part, *homes),
        flops=4 * 10**9,
    )
    from_across = swap(across, 2)
    back = lax.all_to_all(to_owners(force), "flow", split_axis=0, concat_axis=0, tiled=True)
    from_corner = swap(from_across, 1)
    from_beside = swap(beside, 1)
    rows = elements // peers
    total, patch_part = call(
        near_kernel,
        [shape(88, rows), shape(16, 2 * own)],
        scratch=[pltpu.VMEM((176, width), BF16)],
        smem=1,
        operands=(me, beside, from_across, part),
        flops=2 * 10**9,
    )
    flow_force, patch_force = call(
        last_kernel,
        [shape(81, rows), shape(27, own)],
        scratch=[pltpu.VMEM((176, width), BF16)],
        smem=1,
        operands=(me, from_beside, from_corner, total, patch_part),
        flops=2 * 10**9,
    )
    flow_force, pushes = lax.optimization_barrier((flow_force, pushes))
    shell_force = call(
        finish_kernel, shape(3, count),
        scratch=[pltpu.VMEM((owners * 4, slots), F32)],
        operands=(back, block, place, pushes),
        flops=10**8,
    )
    return flow_force, shell_force, patch_force


def solution(mesh):
    both = ("flow", "leaf")
    in_specs = (
        P(None, "flow"), P(both, None), P(both), P(None, both), P(None, both), P(both),
        P(None, both), P(both), P(None, both), P(None, both),
    )
    out_specs = (P(None, both), P(None, both), P(None, both))

    return jax.shard_map(
        per_device, mesh=mesh, in_specs=in_specs, out_specs=out_specs, check_vma=False
    )
```

```python
import functools

import jax
import jax.numpy as jnp
from jax import lax
from jax.experimental import pallas as pl
from jax.experimental.pallas import tpu as pltpu
from jax.sharding import PartitionSpec as P


BETA = 1.5
STIFF = 2.0
REACH = 0.5
BATCH = 2
VMEM_LIMIT = 20 * 2**20
GROUP = 512

F32, BF16, F8 = jnp.float32, jnp.bfloat16, jnp.float8_e4m3fn
I32, I16 = jnp.int32, jnp.int16
NN = (((1,), (0,)), ((), ()))
NT = (((1,), (1,)), ((), ()))


def dot(a, b, dims):
    return lax.dot_general(a, b, dims, preferred_element_type=F32)


def split(x):
    high = x.astype(BF16)
    low = (x - high.astype(F32)).astype(BF16)
    return jnp.concatenate([high, low], axis=0)


def rows_of(shape):
    return lax.broadcasted_iota(I32, shape, 0)


def one_hot(index, rows, offset=0):
    number = lax.broadcasted_iota(I16, (rows, index.shape[1]), 0)
    hit = number == (index - offset).astype(I16)
    return jnp.where(hit, jnp.asarray(1, BF16), jnp.asarray(0, BF16)).astype(F8)


def pick_basis(x, which):
    b0 = 0.5 * (1.0 - x) ** 2
    b1 = 0.5 * (1.0 + 2.0 * x - 2.0 * x * x)
    b2 = 0.5 * x * x
    return jnp.where(which == 0, b0, jnp.where(which == 1, b1, b2))


def split_solid(x):
    high = x[:80].astype(BF16)
    low = (x[:80] - high.astype(F32)).astype(BF16)
    top = x[80:].astype(BF16).astype(F32)
    last = jnp.concatenate([top, x[80:] - top], axis=0).astype(BF16)
    return high, low, last


def join_solid(y):
    return jnp.concatenate([y[:80] + y[80:160], y[160:168] + y[168:176]], axis=0)


def solid_weights(x0, x1, x2):
    j = rows_of((8, 1))
    plane = pick_basis(x1, j // 3) * pick_basis(x2, j % 3)
    corner = (0.5 * x1 * x1) * (0.5 * x2 * x2)
    b0 = 0.5 * (1.0 - x0) ** 2
    b1 = 0.5 * (1.0 + 2.0 * x0 - 2.0 * x0 * x0)
    b2 = 0.5 * x0 * x0
    tiles = [plane * b0, plane * b1, plane * b2]
    return tiles, pick_basis(x0, j % 3) * corner, b2 * corner


def shell_weights(x0, x1):
    k = rows_of((16, 1))
    return pick_basis(x0, k // 3) * pick_basis(x1, k % 3)


def pack_kernel(block_ref, elem_ref, param_ref, vel_ref, weight_ref, out_ref, rank_ref, vals):
    owners, _, slots = out_ref.shape
    count = block_ref.shape[1]
    step = 256
    block = block_ref[...]
    mask = jnp.where(rows_of((owners, count)) == block, 1.0, 0.0)
    upto = (
        lax.broadcasted_iota(I32, (step, step), 0) <= lax.broadcasted_iota(I32, (step, step), 1)
    )
    upto = jnp.where(upto, 1.0, 0.0).astype(BF16)
    base = jnp.zeros((owners, 1), F32)
    ranks = []
    for i in range(count // step):
        part = mask[:, i * step : (i + 1) * step]
        running = dot(part.astype(BF16), upto, NN)
        ranks.append(jnp.sum(part * (running + (base - 1.0)), axis=0, keepdims=True))
        base = base + running[:, step - 1 : step]
    rank = jnp.concatenate(ranks, axis=1).astype(I32)
    rank_ref[...] = rank
    vals[0:1] = elem_ref[...].astype(F32) + 1.0
    vals[1:4] = param_ref[...]
    vals[4:7] = vel_ref[...]
    vals[7:8] = weight_ref[...]
    v = vals[...]
    terms = jnp.concatenate([v * mask[d : d + 1] for d in range(owners)], axis=0)
    packed = dot(split(terms), one_hot(rank, slots), NT)
    packed = packed[: owners * 8] + packed[owners * 8 :]
    for d in range(owners):
        out_ref[d] = packed[d * 8 : (d + 1) * 8]


def contact_kernel(me_ref, *refs, peers):
    ctrl_refs = refs[:peers]
    patch_ref, param_ref, pos_ref, coef_ref, rank_ref = refs[peers : peers + 5]
    push_ref, part_ref, table_ref, place_ref, ctrl, tight, wide = refs[peers + 5 :]
    place_ref[...] = one_hot(rank_ref[...], place_ref.shape[0])
    own = ctrl_refs[0].shape[1]
    me = me_ref[0]
    ctrl[...] = jnp.zeros_like(ctrl)
    for k in range(peers):
        for c in range(3):
            ctrl[c * 16 : c * 16 + 9, k * own : (k + 1) * own] = ctrl_refs[k][c * 9 : c * 9 + 9, :]
    patch = patch_ref[...]
    table = jnp.concatenate([one_hot(patch, own, (me ^ k) * own) for k in range(peers)], axis=0)
    picked = dot(split(ctrl[...]), table, NN)
    picked = picked[:48] + picked[48:]
    w = shell_weights(param_ref[0:1, :], param_ref[1:2, :])
    gaps = [
        pos_ref[c : c + 1, :] - jnp.sum(picked[c * 16 : c * 16 + 16] * w, axis=0, keepdims=True)
        for c in range(3)
    ]
    far = 1.0 + (gaps[0] * gaps[0] + gaps[1] * gaps[1] + gaps[2] * gaps[2]) / (REACH * REACH)
    pushes = [STIFF * g / far for g in gaps]
    for c in range(3):
        push_ref[c : c + 1, :] = pushes[c]
    terms = jnp.concatenate([-(w * f) for f in pushes], axis=0)
    part = dot(split(terms), table, NT)
    part = part[:48] + part[48:]
    for c in range(3):
        tight[c * 9 : c * 9 + 9] = part[c * 16 : c * 16 + 9]
    part_ref[...] = jnp.zeros_like(part_ref)
    for k in range(peers):
        part_ref[k, 0:14, 0:own] = tight[0:14, k * own : (k + 1) * own]
        part_ref[k, 0:13, own:] = tight[14:27, k * own : (k + 1) * own]
    wide[80:88] = jnp.zeros((8, wide.shape[1]), F32)
    for c in range(3):
        for a in range(3):
            k = c * 27 + a * 9
            wide[c * 24 + a * 8 : c * 24 + a * 8 + 8, :] = coef_ref[k : k + 8, :]
            wide[72 + c * 3 + a : 73 + c * 3 + a, :] = coef_ref[k + 8 : k + 9, :]
    table_ref[0:80], table_ref[80:160], table_ref[160:176] = split_solid(wide[...])


def force_of(point, table_ref):
    index = point[0:1].astype(I32) - 1
    picked = join_solid(dot(table_ref[...], one_hot(index, table_ref.shape[1]), NN))
    tiles, rest, final = solid_weights(point[1:2], point[2:3], point[3:4])
    rest = picked[72:80] * rest
    forces = []
    for c in range(3):
        part = jnp.where(rows_of((8, 1)) // 3 == c, rest, 0.0)
        for a in range(3):
            part = part + picked[c * 24 + a * 8 : c * 24 + a * 8 + 8] * tiles[a]
        speed = jnp.sum(part, axis=0, keepdims=True)
        if c == 2:
            speed = speed + picked[80:81] * final
        forces.append(BETA * point[7:8] * (point[4 + c : 5 + c] - speed))
    return forces


def home_kernel(row_ref, sent_ref, table_ref, out_ref):
    for c, force in enumerate(force_of(sent_ref[row_ref[0]], table_ref)):
        out_ref[c : c + 1] = force
    out_ref[3:8] = jnp.zeros((5, GROUP), F32)


def force_kernel(row_ref, recv_ref, table_ref, part_ref, *refs):
    *homes, back_ref, beside_ref, across_ref = refs
    groups = recv_ref.shape[0]

    def put(g, point, forces):
        both = jnp.concatenate([point[0:4], *forces, jnp.zeros((1, GROUP), F32)], axis=0)
        here = pl.ds(pl.multiple_of(g * 8, 8), 8)
        beside_ref[here] = both
        across_ref[here] = both
        back_ref[g] = both[4:8]

    first = row_ref[0]
    order = [lax.rem(first + r, groups) for r in range(groups)]
    if homes:
        put(order[0], recv_ref[order[0]], [homes[0][c : c + 1] for c in range(3)])
        order = order[1:]
    for i in range(0, len(order), BATCH):
        batch = order[i : i + BATCH]
        point = jnp.concatenate([recv_ref[g] for g in batch], axis=1)
        forces = force_of(point, table_ref)
        for j, g in enumerate(batch):
            here = slice(j * GROUP, (j + 1) * GROUP)
            put(g, point[:, here], [f[:, here] for f in forces])
    tail = groups * 8
    beside_ref[tail:] = part_ref[1]
    across_ref[tail : tail + 16] = part_ref[2]
    across_ref[tail + 16 :] = part_ref[3]


def spread(source_ref, terms, first, rows):
    groups = terms.shape[1] // GROUP
    index = []
    for g in range(groups):
        point = source_ref[g * 8 : (g + 1) * 8]
        index.append(point[0:1].astype(I32))
        tiles, rest, final = solid_weights(point[1:2], point[2:3], point[3:4])
        f = [point[4 + c : 5 + c] for c in range(3)]
        which = rows_of((8, 1)) // 3
        parts = [tile * f[c] for c in range(3) for tile in tiles]
        parts.append(rest * jnp.where(which == 0, f[0], jnp.where(which == 1, f[1], f[2])))
        parts.append(jnp.broadcast_to(final * f[2], (8, GROUP)))
        here = pl.ds(g * GROUP, GROUP)
        terms[0:80, here], terms[80:160, here], terms[160:176, here] = split_solid(
            jnp.concatenate(parts, axis=0)
        )
    return dot(terms[...], one_hot(jnp.concatenate(index, axis=1), rows, first), NT)


def near_kernel(me_ref, own_ref, across_ref, part_ref, total_ref, patch_ref, terms):
    rows = total_ref.shape[1]
    tail = terms.shape[1] // GROUP * 8
    first = me_ref[0] * rows + 1
    total = spread(own_ref, terms, first, rows)
    total = total + spread(across_ref, terms, first, rows)
    total_ref[...] = join_solid(total)
    patch_ref[...] = part_ref[0] + across_ref[tail : tail + 16]


def last_kernel(me_ref, beside_ref, corner_ref, total_ref, part_ref, flow_ref, patch_ref, terms):
    rows = total_ref.shape[1]
    own = patch_ref.shape[1]
    tail = terms.shape[1] // GROUP * 8
    first = me_ref[0] * rows + 1
    total = spread(beside_ref, terms, first, rows)
    total = total + spread(corner_ref, terms, first, rows)
    total = total_ref[...] + join_solid(total)
    for c in range(3):
        for a in range(3):
            k = c * 27 + a * 9
            flow_ref[k : k + 8, :] = total[c * 24 + a * 8 : c * 24 + a * 8 + 8]
            flow_ref[k + 8 : k + 9, :] = total[72 + c * 3 + a : 73 + c * 3 + a]
    part = part_ref[...] + beside_ref[tail:] + corner_ref[tail + 16 :]
    patch_ref[0:14] = part[0:14, 0:own]
    patch_ref[14:27] = part[0:13, own:]


def finish_kernel(back_ref, block_ref, place_ref, push_ref, out_ref, rows):
    owners = back_ref.shape[0]
    for d in range(owners):
        rows[d * 4 : (d + 1) * 4] = back_ref[d]
    got = dot(split(rows[...]), place_ref[...], NN)
    got = got[: owners * 4] + got[owners * 4 :]
    block = block_ref[...]
    half = rows_of((8, 1)) // 4
    total = jnp.zeros((8, block.shape[1]), F32)
    for d in range(owners // 2):
        total = total + jnp.where(block - half == 2 * d, got[d * 8 : (d + 1) * 8], 0.0)
    out_ref[...] = push_ref[...] - (total[0:3] + total[4:7])


def call(kernel, out_shape, scratch=(), smem=0, operands=(), flops=0, limit=VMEM_LIMIT):
    specs = [
        pl.BlockSpec(memory_space=pltpu.SMEM if i < smem else pltpu.VMEM)
        for i in range(len(operands))
    ]
    return pl.pallas_call(
        kernel,
        out_shape=out_shape,
        in_specs=specs,
        out_specs=jax.tree.map(lambda _: pl.BlockSpec(memory_space=pltpu.VMEM), out_shape),
        scratch_shapes=scratch,
        cost_estimate=pl.CostEstimate(flops=flops, bytes_accessed=0, transcendentals=0),
        compiler_params=pltpu.CompilerParams(vmem_limit_bytes=limit),
    )(*operands)


def shape(*dims, dtype=F32):
    return jax.ShapeDtypeStruct(dims, dtype)


def per_device(
    vel_coef, gp_block, gp_elem, gp_param, gp_vel, gp_weight, gp_pos, contact_patch,
    contact_param, patch_ctrl,
):
    owners = lax.axis_size("flow")
    peers = lax.axis_size("leaf")
    count = gp_elem.shape[0]
    slots = 2 * count // owners
    width = slots * owners
    groups = width // GROUP
    elements = vel_coef.shape[1]
    own = patch_ctrl.shape[1]
    me = lax.axis_index("leaf").astype(I32).reshape(1)

    def swap(x, k):
        return lax.ppermute(x, "leaf", [(i, i ^ k) for i in range(peers)])

    def to_groups(x):
        if slots == GROUP:
            return x
        return x.transpose(1, 0, 2).reshape(-1, groups, GROUP).transpose(1, 0, 2)

    def to_owners(x):
        if slots == GROUP:
            return x
        return x.transpose(1, 0, 2).reshape(-1, owners, slots).transpose(1, 0, 2)

    block = gp_block.reshape(1, count)
    payload, rank = call(
        pack_kernel,
        [shape(owners, 8, slots), shape(1, count, dtype=I32)],
        scratch=[pltpu.VMEM((8, count), F32)],
        operands=(block, gp_elem.reshape(1, count), gp_param, gp_vel, gp_weight.reshape(1, count)),
        flops=10**9,
        limit=None,
    )
    payload, here = lax.optimization_barrier((payload, patch_ctrl))
    far = swap(here, 2)
    recv = lax.all_to_all(payload, "flow", split_axis=0, concat_axis=0, tiled=True)
    twin = swap(here, 1)
    diag = swap(far, 1)
    ctrl = (here, twin, far, diag)
    pushes, part, table, place = call(
        functools.partial(contact_kernel, peers=peers),
        [
            shape(3, count), shape(peers, 16, 2 * own), shape(176, elements, dtype=BF16),
            shape(slots, count, dtype=F8),
        ],
        scratch=[
            pltpu.VMEM((48, peers * own), F32),
            pltpu.VMEM((32, peers * own), F32),
            pltpu.VMEM((88, elements), F32),
        ],
        smem=1,
        operands=(me, *ctrl, contact_patch.reshape(1, count), contact_param, gp_pos, vel_coef, rank),
        flops=10**9,
    )
    tail = groups * 8
    row = lax.axis_index("flow").astype(I32).reshape(1) % groups
    homes = ()
    if slots == GROUP:
        homes = (
            call(
                home_kernel, shape(8, GROUP), smem=1,
                operands=(row, payload, table), flops=10**9,
            ),
        )
    force, beside, across = call(
        force_kernel,
        [shape(groups, 4, GROUP), shape(tail + 16, GROUP), shape(tail + 32, GROUP)],
        smem=1,
        operands=(row, to_groups(recv), table, part, *homes),
        flops=4 * 10**9,
    )
    from_across = swap(across, 2)
    back = lax.all_to_all(to_owners(force), "flow", split_axis=0, concat_axis=0, tiled=True)
    from_corner = swap(from_across, 1)
    from_beside = swap(beside, 1)
    rows = elements // peers
    total, patch_part = call(
        near_kernel,
        [shape(88, rows), shape(16, 2 * own)],
        scratch=[pltpu.VMEM((176, width), BF16)],
        smem=1,
        operands=(me, beside, from_across, part),
        flops=2 * 10**9,
    )
    flow_force, patch_force = call(
        last_kernel,
        [shape(81, rows), shape(27, own)],
        scratch=[pltpu.VMEM((176, width), BF16)],
        smem=1,
        operands=(me, from_beside, from_corner, total, patch_part),
        flops=2 * 10**9,
    )
    flow_force, pushes = lax.optimization_barrier((flow_force, pushes))
    shell_force = call(
        finish_kernel, shape(3, count),
        scratch=[pltpu.VMEM((owners * 4, slots), F32)],
        operands=(back, block, place, pushes),
        flops=10**8,
    )
    return flow_force, shell_force, patch_force


def solution(mesh):
    both = ("flow", "leaf")
    in_specs = (
        P(None, "flow"), P(both, None), P(both), P(None, both), P(None, both), P(both),
        P(None, both), P(both), P(None, both), P(None, both),
    )
    out_specs = (P(None, both), P(None, both), P(None, both))

    return jax.shard_map(
        per_device, mesh=mesh, in_specs=in_specs, out_specs=out_specs, check_vma=False
    )
```
